128 devices in a mesh: rep: 4 (over y_lo, core), site: 32 (over z, x, y_hi).
Axes of the slice: x: 4, y: 4 (y_hi: 2, y_lo: 2; y = y_hi * 2 + y_lo), z: 4, core: 2. Of those that a mesh axis runs over, the one named last changes fastest.
Arguments:
- working: bfloat16 [4, 32, 16, 64, 2304], P('rep', 'site'), may hold values from -4 to 4
- master_slots: float32 [32, 4, 4, 64, 2304], P('site', 'rep'), may hold values from -4 to 4
- accum_slots: float32 [32, 4, 4, 64, 2304], P('site', 'rep'), may hold values from 0.01 to 1
- pool_images: bfloat16 [4, 256, 32, 1024], P(None, None, 'site'), may hold values from -6 to 6
- pool_targets: bfloat16 [4, 32, 16, 64, 256], P(None, 'site'), may hold values from -0.8984375 to 0.8984375
- batch_index: int32 [4, 3], replicated, may hold values from 0 to 3
- owner_map: int32 [4], replicated, may hold values from 0 to 3, each once
Outputs:
- working_next: bfloat16 [32, 16, 64, 2304], P('site')
- master_next: float32 [32, 4, 4, 64, 2304], P('site', 'rep')
- accum_next: float32 [32, 4, 4, 64, 2304], P('site', 'rep')
The draws below stay inside these ranges and needn't reach their ends.
Inputs may be any that keep to these rules, and one draw needn't show every extreme that they name: `owner_map`: each replica owns exactly one shard.
All inputs are finite; a program needn't handle non-finite values.
Results may differ from the reference program's by a relative error of at most 0.015.
Values may be sent and summed in bfloat16 or wider, within the bound.
A program may use at most 192 MiB of HBM per device.

```python
import math
import jax
import jax.numpy as jnp
from jax import lax

MAPS = 64
CHANNELS = 64
FIELD = 6
SCOLS = 16
BATCH = 256
MICRO = 3
POOL = 4
ROWS = 32
KDIM = 2304
CB = 4
N_REP = 4


def touch_ends(result, own_key, least, largest):
    dims = result.shape
    spot = [jax.random.randint(jax.random.fold_in(own_key, axis), (), 0, dims[axis]) for axis in range(len(dims))]
    result = result.at[tuple(spot)].set(least)
    longest = dims.index(max(dims))
    spot[longest] = (spot[longest] + 1) % dims[longest]
    return result.at[tuple(spot)].set(largest)


def steps_of(rng, extent, shards, smallest, largest):
    factor_of = 1.0
    for axis_at, shards_of in shards:
        heights = jax.random.uniform(jax.random.fold_in(jax.random.fold_in(rng, 6), axis_at), (shards_of,), jnp.float32, smallest / len(shards), largest / len(shards))
        factor_of = factor_of * jnp.repeat(jnp.exp(heights), extent[axis_at] // shards_of).reshape((-1,) + (1,) * (len(extent) - 1 - axis_at))
    return factor_of


def scatter_about(rng, extent, deviation, limit, cuts=(), kind=jnp.bfloat16):
    values = deviation * jax.random.normal(rng, extent, jnp.float32)
    if cuts:
        values = values * steps_of(rng, extent, cuts, -0.22, 0.18)
    return jnp.clip(values, -limit, limit).astype(kind)


def setup_inputs(seed: int = 0) -> dict:
    seeds = jax.random.split(jax.random.key(seed), 8)
    working = scatter_about(seeds[0], (N_REP, ROWS, SCOLS, MAPS, KDIM), 1.0, 4.0, ((0, 4), (1, 32)))
    master_slots = scatter_about(seeds[1], (ROWS, N_REP, CB, MAPS, KDIM), 1.0, 4.0, ((0, 32), (1, 4)), jnp.float32)
    accum_slots = jnp.clip(jnp.exp(math.log(1.0) - 4.6051702 * jax.random.uniform(seeds[2], (ROWS, N_REP, CB, MAPS, KDIM), jnp.float32) ** steps_of(seeds[2], (ROWS, N_REP, CB, MAPS, KDIM), ((0, 32), (1, 4)), -0.2, 0.2)), 0.01, 1.0)
    pool_images = scatter_about(seeds[3], (POOL, BATCH, ROWS, SCOLS * CHANNELS), 1.0, 6.0, ((2, 32),))
    pool_targets = jnp.clip(jax.random.uniform(seeds[4], (POOL, ROWS, SCOLS, MAPS, BATCH), jnp.float32, -0.8984375, 0.8984375) * steps_of(seeds[4], (POOL, ROWS, SCOLS, MAPS, BATCH), ((1, 32),), -0.4, 0.0), -0.8984375, 0.8984375).astype(jnp.bfloat16)
    batch_index = touch_ends(jax.random.randint(seeds[5], (N_REP, MICRO), 0, POOL), jax.random.fold_in(seeds[5], 1), 0, POOL - 1).astype(jnp.int32)
    owner_map = jax.random.permutation(seeds[6], N_REP).astype(jnp.int32)
    return dict(working=working, master_slots=master_slots, accum_slots=accum_slots, pool_images=pool_images, pool_targets=pool_targets, batch_index=batch_index, owner_map=owner_map)


learning_rate = 0.3
epsilon = 1e-08

def build_patches(window):
    batch_rows = window.shape[0]
    columns = window.shape[2] // CHANNELS
    grid_cells = window.reshape(batch_rows, FIELD, columns, CHANNELS)
    padded = jnp.pad(grid_cells, ((0, 0), (0, 0), (2, 3), (0, 0)))
    stacked = jnp.stack([padded[:, :, offset:offset + columns, :] for offset in range(FIELD)], axis=2)
    return stacked.transpose(0, 3, 1, 2, 4).reshape(batch_rows, columns, FIELD * FIELD * CHANNELS)

def replica_gradient(weights, chosen, pool_images, pool_targets):
    factor = (FIELD * FIELD * CHANNELS) ** (-0.5)
    total = jnp.zeros(weights.shape, jnp.float32)
    for micro_step in range(MICRO):
        images = lax.dynamic_index_in_dim(pool_images, chosen[micro_step], 0, keepdims=False)
        targets = lax.dynamic_index_in_dim(pool_targets, chosen[micro_step], 0, keepdims=False)
        padded = jnp.pad(images, ((0, 0), (2, 3), (0, 0)))

        def row_gradient(site_row):
            window = lax.dynamic_slice_in_dim(padded, site_row, FIELD, 1)
            patches = build_patches(window).astype(jnp.float32)
            row_weights = lax.dynamic_index_in_dim(weights, site_row, 0, keepdims=False).astype(jnp.float32)
            row_targets = lax.dynamic_index_in_dim(targets, site_row, 0, keepdims=False).astype(jnp.float32)
            forward = factor * jnp.einsum('bck,cok->cob', patches, row_weights)
            active = jnp.tanh(forward)
            signal = ((active - row_targets) * (1.0 - active * active)).astype(jnp.bfloat16)
            signal = lax.optimization_barrier(signal).astype(jnp.float32)
            return factor * jnp.einsum('cob,bck->cok', signal, patches)
        total = total + lax.map(row_gradient, jnp.arange(ROWS, dtype=jnp.int32))
    return total

def reference(working, master_slots, accum_slots, pool_images, pool_targets, batch_index, owner_map):
    total = jnp.zeros((ROWS, SCOLS, MAPS, FIELD * FIELD * CHANNELS), jnp.float32)
    for replica in range(N_REP):
        partial_grad = replica_gradient(working[replica], batch_index[replica], pool_images, pool_targets)
        rounded = lax.optimization_barrier(partial_grad.astype(jnp.bfloat16))
        total = total + rounded.astype(jnp.float32)
    blocks = total.reshape(ROWS, N_REP, SCOLS // N_REP, MAPS, FIELD * FIELD * CHANNELS)
    slot_grad = jnp.take(blocks, owner_map, axis=1)
    accum_next = accum_slots + slot_grad * slot_grad
    master_next = master_slots - learning_rate * slot_grad / (jnp.sqrt(accum_next) + epsilon)
    numbers = jnp.arange(N_REP, dtype=jnp.int32)
    matches = (owner_map[:, None] == numbers[None, :]).astype(jnp.int32)
    inverse = lax.optimization_barrier(jnp.sum(numbers[:, None] * matches, axis=0))
    working_next = jnp.take(master_next.astype(jnp.bfloat16), inverse, axis=1)
    working_next = working_next.reshape(ROWS, SCOLS, MAPS, FIELD * FIELD * CHANNELS)
    return (working_next, master_next, accum_next)
```

```python
import functools

import jax
import jax.numpy as jnp
from jax import lax
from jax.experimental import pallas as pl
from jax.experimental.pallas import tpu as pltpu
from jax.sharding import PartitionSpec as P

MICRO = 3
POOL = 4
FIELD = 6
REPS = 4
CB = 4
CH = 64
MAPS = 64
TAPS = FIELD * CH
BAND = 640
LEFT = 128
HALVES = 2
OWN = 2
FACTOR = (FIELD * FIELD * CH) ** (-0.5)
LEARNING_RATE = 0.3
EPSILON = 1e-08

MESH = pl.DeviceIdType.MESH


def step_kernel(
    sites,
    pick_ref,
    count_ref,
    images_ref,
    targets_ref,
    working_ref,
    master_ref,
    accum_ref,
    fetched_ref,
    master_out,
    accum_out,
    x0,
    x1,
    x2,
    x3,
    x4,
    x5,
    weights,
    banded,
    targets,
    signal,
    chosen,
    chosen_in,
    kept,
    own,
    pair,
    pair_in,
    combined,
    window,
    master,
    accum,
    mine,
    theirs,
    grad,
    sem_load,
    send_a,
    send_b,
    send_c,
    send_d,
    send_e,
    send_f,
    send_g,
    send_x,
    recv_l,
    recv_x,
    send_s,
    recv_s,
    send_p,
    recv_p,
    send_w,
    recv_w,
    sem_store,
):
    x = [x0, x1, x2, x3, x4, x5]
    batch = images_ref.shape[1]
    width = images_ref.shape[2]
    piece = batch // HALVES
    duo = 2 * piece
    span = POOL * piece

    g = lax.axis_index("rep")
    s = lax.axis_index("site")
    side = g // 2
    core = g % 2
    odd = s % 2
    even = odd == 0

    def peer(k):
        return 2 * ((side + k // 2) % 2) + (core + k % 2) % 2

    ahead = (g, s + 2)
    behind = (g, s - 2)
    across = (2 * (1 - side) + core, s + 1 - 2 * odd)
    partner = (2 * (1 - side) + core, s)
    sibling = (2 * side + 1 - core, s)
    has_ahead = s + 2 < sites
    has_behind = s >= 2
    valid = [(s + d - 2 >= 0) & (s + d - 2 < sites) for d in range(FIELD)]
    halves = range(HALVES)

    def own_image(p, h):
        return pltpu.make_async_copy(
            images_ref.at[p, pl.ds(h * piece, piece)],
            x[OWN].at[pl.ds(h * span + p * piece, piece), pl.ds(LEFT, width)],
            sem_load.at[p, h],
        )

    loads = [
        pltpu.make_async_copy(working_ref, weights, sem_load.at[POOL, 0]),
        pltpu.make_async_copy(targets_ref, targets, sem_load.at[POOL + 1, 0]),
        pltpu.make_async_copy(master_ref, master, sem_load.at[POOL + 2, 0]),
        pltpu.make_async_copy(accum_ref, accum, sem_load.at[POOL + 3, 0]),
    ]
    for h in halves:
        for p in range(POOL):
            own_image(p, h).start()
    for load in loads:
        load.start()

    right = x[0].shape[1] - LEFT - width
    for d in range(FIELD):
        x[d][:, 0:LEFT] = jnp.zeros((POOL * batch, LEFT), jnp.bfloat16)
        x[d][:, LEFT + width :] = jnp.zeros((POOL * batch, right), jnp.bfloat16)
        if d != OWN:

            @pl.when(jnp.logical_not(valid[d]))
            def _(d=d):
                x[d][:, LEFT : LEFT + width] = jnp.zeros((POOL * batch, width), jnp.bfloat16)

    barrier = pltpu.get_barrier_semaphore()
    for device in (across, partner, sibling):
        pl.semaphore_signal(barrier, inc=1, device_id=device, device_id_type=MESH)

    @pl.when(has_ahead)
    def _():
        pl.semaphore_signal(barrier, inc=1, device_id=ahead, device_id_type=MESH)

    @pl.when(has_behind)
    def _():
        pl.semaphore_signal(barrier, inc=1, device_id=behind, device_id_type=MESH)

    pl.semaphore_wait(barrier, 3 + has_ahead.astype(jnp.int32) + has_behind.astype(jnp.int32))

    q = (2 * core + side, 2 * core + 1 - side)

    def rows(slot, p, h):
        return x[slot].at[
            pl.ds(pl.multiple_of(h * span + p * piece, piece), piece), pl.ds(LEFT, width)
        ]

    def link(src, dst, p, h, device, sem):
        return pltpu.make_async_remote_copy(
            src_ref=rows(src, p, h),
            dst_ref=rows(dst, p, h),
            send_sem=sem,
            recv_sem=recv_l.at[dst, p % 2, h],
            device_id=device,
            device_id_type=MESH,
        )

    def hand_over(slot, p, h):
        return pltpu.make_async_remote_copy(
            src_ref=rows(slot, p, h),
            dst_ref=rows(slot, p, h),
            send_sem=send_x.at[slot, p % 2, h],
            recv_sem=recv_x.at[slot, p % 2, h],
            device_id=sibling,
            device_id_type=MESH,
        )

    def natives(h):
        for p in range(POOL):
            own_image(p, h).wait()

        @pl.when(has_ahead)
        def _():
            for i in (0, 1):
                link(OWN, 0, q[i], h, ahead, send_a.at[i, h]).start()

        @pl.when(has_behind)
        def _():
            for i in (1, 0):
                link(OWN, 4, q[i], h, behind, send_b.at[i, h]).start()

        @pl.when(even)
        def _():
            link(OWN, 1, q[0], h, across, send_c.at[0, h]).start()

            @pl.when(s == 0)
            def _():
                link(OWN, 1, q[1], h, across, send_c.at[1, h]).start()

        @pl.when(odd == 1)
        def _():
            for i in (1, 0):
                link(OWN, 3, q[i], h, across, send_c.at[i, h]).start()

    def passed(slot, p, h, *sends):
        @pl.when(valid[slot])
        def _():
            link(slot, slot, p, h, partner, send_a.at[0, 0]).wait_recv()
            for condition, copy in sends:

                @pl.when(condition)
                def _(copy=copy):
                    copy.start()

            hand_over(slot, p, h).start()

    def onward(h):
        return (
            (has_ahead, link(3, 1, q[0], h, ahead, send_e.at[h])),
            (has_behind, link(3, 5, q[0], h, behind, send_f.at[h])),
        )

    def swap(h):
        return (valid[5], link(5, 5, q[0], h, partner, send_g.at[h]))

    def arrivals_one(h):
        @pl.when(even)
        def _():
            passed(4, q[1], h, (has_ahead, link(4, 3, q[1], h, across, send_d.at[1, h])))
            passed(3, q[0], h, *onward(h))
            passed(0, q[0], h)

        @pl.when(odd == 1)
        def _():
            passed(0, q[0], h, (has_behind, link(0, 1, q[0], h, across, send_d.at[0, h])))
            passed(4, q[1], h)
            passed(1, q[1], h)

    def arrivals_two(h):
        @pl.when(even)
        def _():
            passed(4, q[0], h, (has_ahead, link(4, 3, q[0], h, across, send_d.at[0, h])))
            passed(3, q[1], h)
            passed(0, q[1], h)

        @pl.when(odd == 1)
        def _():
            passed(3, q[0], h, *onward(h))
            passed(4, q[0], h)
            passed(0, q[1], h)

    def arrivals_three(h):
        passed(5, q[0], h, swap(h))
        passed(1, q[0], h)

        @pl.when(even)
        def _():
            passed(1, q[1], h)

        @pl.when(odd == 1)
        def _():
            passed(3, q[1], h)

        passed(5, q[1], h)
        for slot in (0, 1, 3, 4, 5):

            @pl.when(valid[slot])
            def _(slot=slot):
                for j in range(2):
                    pltpu.make_async_remote_copy(
                        src_ref=rows(slot, 2 * (1 - core) + j, h),
                        dst_ref=rows(slot, 2 * (1 - core) + j, h),
                        send_sem=send_x.at[slot, j, h],
                        recv_sem=recv_x.at[slot, j, h],
                        device_id=sibling,
                        device_id_type=MESH,
                    ).wait_recv()

    def band_weights(block, carry):
        for cc in range(CB):
            for d in range(FIELD):
                taps = weights[block * CB + cc, :, d * TAPS : (d + 1) * TAPS]
                if cc % 2:
                    wide = jnp.concatenate(
                        [taps.astype(jnp.float32), jnp.zeros((MAPS, LEFT), jnp.float32)], axis=1
                    )
                    taps = pltpu.roll(wide, CH, 1).astype(jnp.bfloat16)
                before = (cc // 2) * LEFT
                after = BAND - before - taps.shape[1]
                parts = [taps]
                if before:
                    parts = [jnp.zeros((MAPS, before), jnp.bfloat16)] + parts
                if after:
                    parts = parts + [jnp.zeros((MAPS, after), jnp.bfloat16)]
                banded[block, cc * MAPS : (cc + 1) * MAPS, d * BAND : (d + 1) * BAND] = (
                    jnp.concatenate(parts, axis=1)
                )
        return carry

    def forward(h, n, low, high):
        at = h * span + n * duo

        def one_block(block, carry):
            lanes = pl.multiple_of(block * (CB * CH), CB * CH)
            total = jnp.zeros((CB * MAPS, duo), jnp.float32)
            for d in range(FIELD):
                total = total + lax.dot_general(
                    banded[block, :, d * BAND : (d + 1) * BAND],
                    x[d][at : at + duo, pl.ds(lanes, BAND)],
                    (((1,), (1,)), ((), ())),
                    preferred_element_type=jnp.float32,
                )
            active = jnp.tanh(FACTOR * total)
            of_block = pl.ds(pl.multiple_of(block * (CB * MAPS), CB * MAPS), CB * MAPS)
            of_half = slice(h * piece, (h + 1) * piece)
            wanted = jnp.concatenate(
                [targets[2 * n, of_block, of_half], targets[2 * n + 1, of_block, of_half]], axis=1
            ).astype(jnp.float32)
            signal[block] = ((active - wanted) * (1.0 - active * active)).astype(jnp.bfloat16)
            return carry

        lax.fori_loop(low, high, one_block, 0)

    strip = 32

    def select(h, n):
        def one_strip(i, carry):
            at = pl.ds(pl.multiple_of(i * strip, strip), strip)
            parts = [signal[block, at, :] for block in range(REPS)]
            results = []
            for k in range(REPS):
                taken = None
                for block in range(REPS):
                    scale = jnp.full((strip, duo), pick_ref[peer(k), block], jnp.float32)
                    term = scale.astype(jnp.bfloat16) * parts[block]
                    taken = term if taken is None else taken + term
                results.append(taken)
            own[h, n, at, :] = results[0]
            chosen[h, n, 0, at, :] = results[1]
            kept[h, n, at, :] = results[2]
            chosen[h, n, 1, at, :] = results[3]
            return carry

        lax.fori_loop(0, CB * MAPS // strip, one_strip, 0)

    def choice(h, n):
        return pltpu.make_async_remote_copy(
            src_ref=chosen.at[h, n],
            dst_ref=chosen_in.at[h, n],
            send_sem=send_s.at[h, n],
            recv_sem=recv_s.at[h, n],
            device_id=sibling,
            device_id_type=MESH,
        )

    def pair_copy(h, n):
        return pltpu.make_async_remote_copy(
            src_ref=pair.at[h, n],
            dst_ref=pair_in.at[h, n],
            send_sem=send_p.at[h, n],
            recv_sem=recv_p.at[h, n],
            device_id=partner,
            device_id_type=MESH,
        )

    def weighed(k, n, value):
        value = value.astype(jnp.float32)
        return jnp.concatenate(
            [
                count_ref[peer(k), 2 * n] * value[:, :piece],
                count_ref[peer(k), 2 * n + 1] * value[:, piece:],
            ],
            axis=1,
        )

    def make_pair(h, n):
        choice(h, n).wait_recv()

        def one_strip(i, carry):
            at = pl.ds(pl.multiple_of(i * strip, strip), strip)
            pair[h, n, at, :] = (
                weighed(0, n, kept[h, n, at, :]) + weighed(1, n, chosen_in[h, n, 1, at, :])
            ).astype(jnp.bfloat16)
            return carry

        lax.fori_loop(0, CB * MAPS // strip, one_strip, 0)
        pair_copy(h, n).start()

    def combine(h, n):
        pair_copy(h, n).wait_recv()
        lanes = slice(h * span + n * duo, h * span + (n + 1) * duo)

        def one_strip(i, carry):
            at = pl.ds(pl.multiple_of(i * strip, strip), strip)
            combined[at, lanes] = (
                weighed(0, n, own[h, n, at, :])
                + weighed(1, n, chosen_in[h, n, 0, at, :])
                + pair_in[h, n, at, :].astype(jnp.float32)
            ).astype(jnp.bfloat16)
            return carry

        lax.fori_loop(0, CB * MAPS // strip, one_strip, 0)

    def own_window(h):
        def one_strip(i, carry):
            at = pl.ds(pl.multiple_of(h * span + i * strip, strip), strip)
            for d in range(FIELD):
                taken = None
                for block in range(REPS):
                    scale = jnp.full((strip, BAND), pick_ref[g, block], jnp.float32)
                    lanes = slice(block * CB * CH, block * CB * CH + BAND)
                    term = scale.astype(jnp.bfloat16) * x[d][at, lanes]
                    taken = term if taken is None else taken + term
                window[d, at, :] = taken
            return carry

        lax.fori_loop(0, span // strip, one_strip, 0)

    natives(0)
    loads[0].wait()
    lax.fori_loop(0, REPS, band_weights, 0)
    for load in loads[1:]:
        load.wait()
    arrivals_one(0)
    arrivals_two(0)
    natives(1)
    arrivals_three(0)
    forward(0, 0, 0, REPS)
    select(0, 0)
    choice(0, 0).start()
    arrivals_one(1)
    forward(0, 1, 0, REPS)
    make_pair(0, 0)
    select(0, 1)
    choice(0, 1).start()
    arrivals_two(1)
    make_pair(0, 1)
    own_window(0)
    combine(0, 0)
    combine(0, 1)
    arrivals_three(1)
    forward(1, 0, 0, REPS)
    select(1, 0)
    choice(1, 0).start()
    forward(1, 1, 0, REPS // 2)
    make_pair(1, 0)
    forward(1, 1, REPS // 2, REPS)
    select(1, 1)
    choice(1, 1).start()
    own_window(1)
    make_pair(1, 1)
    combine(1, 0)
    combine(1, 1)

    def part_of(ref, d):
        return ref.at[:, :, pl.ds(d * TAPS, TAPS)]

    def send_across(d):
        return pltpu.make_async_remote_copy(
            src_ref=part_of(mine, d),
            dst_ref=part_of(theirs, d),
            send_sem=send_w.at[0, d],
            recv_sem=recv_w.at[0, d],
            device_id=partner,
            device_id_type=MESH,
        )

    def send_beside(d):
        return pltpu.make_async_remote_copy(
            src_ref=part_of(mine, d),
            dst_ref=part_of(fetched_ref.at[1], d),
            send_sem=send_w.at[1, d],
            recv_sem=recv_w.at[1, d],
            device_id=sibling,
            device_id_type=MESH,
        )

    def pass_beside(d):
        return pltpu.make_async_remote_copy(
            src_ref=part_of(theirs, d),
            dst_ref=part_of(fetched_ref.at[3], d),
            send_sem=send_w.at[2, d],
            recv_sem=recv_w.at[2, d],
            device_id=sibling,
            device_id_type=MESH,
        )

    def stores(d):
        return [
            pltpu.make_async_copy(
                part_of(mine, d), part_of(fetched_ref.at[0], d), sem_store.at[0, d]
            ),
            pltpu.make_async_copy(part_of(master, d), part_of(master_out, d), sem_store.at[1, d]),
            pltpu.make_async_copy(part_of(accum, d), part_of(accum_out, d), sem_store.at[2, d]),
        ]

    def store_theirs(d):
        return pltpu.make_async_copy(
            part_of(theirs, d), part_of(fetched_ref.at[2], d), sem_store.at[3, d]
        )

    def send_part(d):
        send_across(d).start()
        send_beside(d).start()
        for store in stores(d):
            store.start()

    for d in range(FIELD):
        for at in range(0, BAND, 256):
            wide = min(256, BAND - at)
            grad[:, at : at + wide] = jnp.dot(
                combined[...],
                window[d, :, at : at + wide],
                preferred_element_type=jnp.float32,
            )
        if d:
            send_part(d - 1)
        for cc in range(CB):
            before = (cc // 2) * LEFT
            of_column = slice(cc * MAPS, (cc + 1) * MAPS)
            if cc % 2:
                wide = grad[of_column, before : before + TAPS + LEFT]
                column = pltpu.roll(wide, TAPS + LEFT - CH, 1)[:, :TAPS]
            else:
                column = grad[of_column, before : before + TAPS]
            slot_grad = FACTOR * column
            taps = slice(d * TAPS, (d + 1) * TAPS)
            accum_next = accum[cc, :, taps] + slot_grad * slot_grad
            master_next = master[cc, :, taps] - LEARNING_RATE * slot_grad / (
                jnp.sqrt(accum_next) + EPSILON
            )
            accum[cc, :, taps] = accum_next
            master[cc, :, taps] = master_next
            mine[cc, :, taps] = master_next.astype(jnp.bfloat16)

    send_part(FIELD - 1)
    for d in range(FIELD):
        send_across(d).wait_recv()
        pass_beside(d).start()
        store_theirs(d).start()

    for d in range(FIELD):
        send_across(d).wait_send()
        send_beside(d).wait()
        for store in stores(d):
            store.wait()
        store_theirs(d).wait()
        pass_beside(d).wait()
    for h in halves:
        for n in range(POOL // 2):
            choice(h, n).wait_send()
            pair_copy(h, n).wait_send()

    def all_sent(condition, sems):
        @pl.when(condition)
        def _():
            for sem in sems:
                link(OWN, OWN, 0, 0, partner, sem).wait_send()

    all_sent(has_ahead, [send_a.at[i, h] for i in (0, 1) for h in halves])
    all_sent(has_behind, [send_b.at[i, h] for i in (0, 1) for h in halves])
    all_sent(s >= 0, [send_c.at[0, h] for h in halves])
    all_sent((odd == 1) | (s == 0), [send_c.at[1, h] for h in halves])
    all_sent((even & has_ahead) | ((odd == 1) & has_behind), [send_d.at[0, h] for h in halves])
    all_sent(even & has_ahead, [send_d.at[1, h] for h in halves])
    all_sent(has_ahead, [send_e.at[h] for h in halves])
    all_sent(has_behind & valid[3], [send_f.at[h] for h in halves])
    all_sent(valid[5], [send_g.at[h] for h in halves])
    for slot in (0, 1, 3, 4, 5):
        all_sent(valid[slot], [send_x.at[slot, j, h] for j in (0, 1) for h in halves])


def per_device(
    working, master_slots, accum_slots, pool_images, pool_targets, batch_index, owner_map
):
    sites = lax.axis_size("site")
    batch = pool_images.shape[1]
    width = pool_images.shape[3]
    weights = working[0, 0]
    columns, maps, kdim = weights.shape
    padded = width - CB * CH + BAND
    duo = 2 * (batch // HALVES)
    me = lax.axis_index("rep")
    numbers = jnp.arange(REPS, dtype=jnp.int32)
    pick = (owner_map[:, None] == numbers).astype(jnp.float32)
    count = jnp.sum((batch_index[:, :, None] == numbers).astype(jnp.float32), axis=1)
    any_space = pl.BlockSpec(memory_space=pl.ANY)
    smem = pl.BlockSpec(memory_space=pltpu.SMEM)
    dma = pltpu.SemaphoreType.DMA
    fetched, master_next, accum_next = pl.pallas_call(
        functools.partial(step_kernel, sites),
        out_shape=(
            jax.ShapeDtypeStruct((REPS, CB, maps, kdim), jnp.bfloat16),
            jax.ShapeDtypeStruct((CB, maps, kdim), jnp.float32),
            jax.ShapeDtypeStruct((CB, maps, kdim), jnp.float32),
        ),
        in_specs=[smem, smem] + [any_space] * 5,
        out_specs=(any_space, any_space, any_space),
        scratch_shapes=[pltpu.VMEM((POOL * batch, padded), jnp.bfloat16)] * FIELD
        + [
            pltpu.VMEM((columns, maps, kdim), jnp.bfloat16),
            pltpu.VMEM((REPS, CB * maps, FIELD * BAND), jnp.bfloat16),
            pltpu.VMEM((POOL, columns * maps, batch), jnp.bfloat16),
            pltpu.VMEM((REPS, CB * maps, duo), jnp.bfloat16),
            pltpu.VMEM((HALVES, 2, 2, CB * maps, duo), jnp.bfloat16),
            pltpu.VMEM((HALVES, 2, 2, CB * maps, duo), jnp.bfloat16),
            pltpu.VMEM((HALVES, 2, CB * maps, duo), jnp.bfloat16),
            pltpu.VMEM((HALVES, 2, CB * maps, duo), jnp.bfloat16),
            pltpu.VMEM((HALVES, 2, CB * maps, duo), jnp.bfloat16),
            pltpu.VMEM((HALVES, 2, CB * maps, duo), jnp.bfloat16),
            pltpu.VMEM((CB * maps, POOL * batch), jnp.bfloat16),
            pltpu.VMEM((FIELD, POOL * batch, BAND), jnp.bfloat16),
            pltpu.VMEM((CB, maps, kdim), jnp.float32),
            pltpu.VMEM((CB, maps, kdim), jnp.float32),
            pltpu.VMEM((CB, maps, kdim), jnp.bfloat16),
            pltpu.VMEM((CB, maps, kdim), jnp.bfloat16),
            pltpu.VMEM((CB * maps, BAND), jnp.float32),
            dma((POOL + 4, HALVES)),
            dma((2, HALVES)),
            dma((2, HALVES)),
            dma((2, HALVES)),
            dma((2, HALVES)),
            dma((HALVES,)),
            dma((HALVES,)),
            dma((HALVES,)),
            dma((FIELD, 2, HALVES)),
            dma((FIELD, 2, HALVES)),
            dma((FIELD, 2, HALVES)),
            dma((HALVES, 2)),
            dma((HALVES, 2)),
            dma((HALVES, 2)),
            dma((HALVES, 2)),
            dma((3, FIELD)),
            dma((3, FIELD)),
            dma((4, FIELD)),
        ],
        compiler_params=pltpu.CompilerParams(
            collective_id=0, has_side_effects=True, vmem_limit_bytes=62 * 1024 * 1024
        ),
        name="step",
    )(
        pick,
        count,
        pool_images[:, :, 0, :],
        pool_targets.reshape(POOL, columns * maps, batch),
        weights,
        master_slots[0, 0],
        accum_slots[0, 0],
    )
    matches = (owner_map[:, None] == numbers[None, :]).astype(jnp.int32)
    owner_of = jnp.sum(numbers[:, None] * matches, axis=0)
    working_next = jnp.take(fetched, owner_of ^ me, axis=0, mode="clip").reshape(weights.shape)[None]
    return (working_next, master_next[None, None], accum_next[None, None])


def solution(mesh):
    placed = (
        P("rep", "site", None, None, None),
        P("site", "rep", None, None, None),
        P("site", "rep", None, None, None),
        P(None, None, "site", None),
        P(None, "site", None, None, None),
        P(),
        P(),
    )
    return jax.shard_map(
        per_device,
        mesh=mesh,
        in_specs=placed,
        out_specs=(
            P("site", None, None, None),
            P("site", "rep", None, None, None),
            P("site", "rep", None, None, None),
        ),
        check_vma=False,
    )
```

```python
import functools

import jax
import jax.numpy as jnp
from jax import lax
from jax.experimental import pallas as pl
from jax.experimental.pallas import tpu as pltpu
from jax.sharding import PartitionSpec as P

MICRO = 3
POOL = 4
FIELD = 6
REPS = 4
CB = 4
CH = 64
MAPS = 64
TAPS = FIELD * CH
BAND = 640
LEFT = 128
PIECES = 4
OWN = 2
FACTOR = (FIELD * FIELD * CH) ** (-0.5)
LEARNING_RATE = 0.3
EPSILON = 1e-08

MESH = pl.DeviceIdType.MESH


def step_kernel(
    sites,
    index_ref,
    owner_ref,
    images_ref,
    targets_ref,
    working_ref,
    master_ref,
    accum_ref,
    fetched_ref,
    master_out,
    accum_out,
    x0,
    x1,
    x2,
    x3,
    x4,
    x5,
    weights,
    banded,
    targets,
    signal,
    chosen,
    chosen_in,
    kept,
    own,
    pair,
    pair_in,
    combined,
    window,
    master,
    accum,
    mine,
    theirs,
    grad,
    sem_load,
    send_a,
    send_b,
    send_c,
    send_d,
    send_e,
    send_f,
    send_g,
    send_x,
    recv_l,
    recv_x,
    send_s,
    recv_s,
    send_p,
    recv_p,
    send_w,
    recv_w,
    sem_store,
):
    x = [x0, x1, x2, x3, x4, x5]
    batch = images_ref.shape[1]
    width = images_ref.shape[2]
    piece = batch // PIECES
    span = POOL * piece

    g = lax.axis_index("rep")
    s = lax.axis_index("site")
    side = g // 2
    core = g % 2
    odd = s % 2
    even = odd == 0

    def peer(k):
        return 2 * ((side + k // 2) % 2) + (core + k % 2) % 2

    ahead = (g, s + 2)
    behind = (g, s - 2)
    across = (2 * (1 - side) + core, s + 1 - 2 * odd)
    partner = (2 * (1 - side) + core, s)
    sibling = (2 * side + 1 - core, s)
    has_ahead = s + 2 < sites
    has_behind = s >= 2
    valid = [(s + d - 2 >= 0) & (s + d - 2 < sites) for d in range(FIELD)]

    def same(a, b):
        return (1 - jnp.minimum(jnp.abs(a - b), 1)).astype(jnp.float32)

    pick = [[same(owner_ref[peer(k)], block) for block in range(REPS)] for k in range(REPS)]
    entry = lax.broadcasted_iota(jnp.int32, (1, span), 1) // piece
    count = []
    for k in range(2):
        of_lane = jnp.zeros((1, span), jnp.float32)
        for p in range(POOL):
            times = sum(same(index_ref[peer(k), m], p) for m in range(MICRO))
            of_lane = jnp.where(entry == p, times, of_lane)
        count.append(of_lane)

    barrier = pltpu.get_barrier_semaphore()
    for device in (across, partner, sibling):
        pl.semaphore_signal(barrier, inc=1, device_id=device, device_id_type=MESH)

    @pl.when(has_ahead)
    def _():
        pl.semaphore_signal(barrier, inc=1, device_id=ahead, device_id_type=MESH)

    @pl.when(has_behind)
    def _():
        pl.semaphore_signal(barrier, inc=1, device_id=behind, device_id_type=MESH)

    def own_image(p, h):
        return pltpu.make_async_copy(
            images_ref.at[p, pl.ds(h * piece, piece)],
            x[OWN].at[pl.ds(h * span + p * piece, piece), pl.ds(LEFT, width)],
            sem_load.at[p, h],
        )

    loads = [
        pltpu.make_async_copy(working_ref, weights, sem_load.at[POOL, 0]),
        pltpu.make_async_copy(targets_ref, targets, sem_load.at[POOL + 1, 0]),
        pltpu.make_async_copy(master_ref, master, sem_load.at[POOL + 2, 0]),
        pltpu.make_async_copy(accum_ref, accum, sem_load.at[POOL + 3, 0]),
    ]
    for h in range(PIECES):
        for p in range(POOL):
            own_image(p, h).start()
    for load in loads:
        load.start()

    right = x[0].shape[1] - LEFT - width
    for d in range(FIELD):
        x[d][:, 0:LEFT] = jnp.zeros((POOL * batch, LEFT), jnp.bfloat16)
        x[d][:, LEFT + width :] = jnp.zeros((POOL * batch, right), jnp.bfloat16)
        if d != OWN:

            @pl.when(jnp.logical_not(valid[d]))
            def _(d=d):
                x[d][:, LEFT : LEFT + width] = jnp.zeros((POOL * batch, width), jnp.bfloat16)

    pl.semaphore_wait(barrier, 3 + has_ahead.astype(jnp.int32) + has_behind.astype(jnp.int32))

    q = (2 * core + side, 2 * core + 1 - side)

    def rows(slot, p, h):
        return x[slot].at[
            pl.ds(pl.multiple_of(h * span + p * piece, piece), piece), pl.ds(LEFT, width)
        ]

    def link(src, dst, p, h, device, sem):
        return pltpu.make_async_remote_copy(
            src_ref=rows(src, p, h),
            dst_ref=rows(dst, p, h),
            send_sem=sem,
            recv_sem=recv_l.at[dst, p % 2, h],
            device_id=device,
            device_id_type=MESH,
        )

    def hand_over(slot, p, h):
        return pltpu.make_async_remote_copy(
            src_ref=rows(slot, p, h),
            dst_ref=rows(slot, p, h),
            send_sem=send_x.at[slot, p % 2, h],
            recv_sem=recv_x.at[slot, p % 2, h],
            device_id=sibling,
            device_id_type=MESH,
        )

    def natives():
        for h in range(PIECES):
            for p in range(POOL):
                own_image(p, h).wait()

        @pl.when(has_ahead)
        def _():
            for i in (0, 1):
                for h in range(PIECES):
                    link(OWN, 0, q[i], h, ahead, send_a.at[i, h]).start()

        @pl.when(has_behind)
        def _():
            for i in (1, 0):
                for h in range(PIECES):
                    link(OWN, 4, q[i], h, behind, send_b.at[i, h]).start()

        @pl.when(even)
        def _():
            for h in range(PIECES):
                link(OWN, 1, q[0], h, across, send_c.at[0, h]).start()

            @pl.when(s == 0)
            def _():
                for h in range(PIECES):
                    link(OWN, 1, q[1], h, across, send_c.at[1, h]).start()

        @pl.when(odd == 1)
        def _():
            for i in (1, 0):
                for h in range(PIECES):
                    link(OWN, 3, q[i], h, across, send_c.at[i, h]).start()

    def passed(slot, p, h, *sends):
        @pl.when(valid[slot])
        def _():
            link(slot, slot, p, h, partner, send_a.at[0, 0]).wait_recv()
            for condition, copy in sends:

                @pl.when(condition)
                def _(copy=copy):
                    copy.start()

            hand_over(slot, p, h).start()

    def onward(h):
        return (
            (has_ahead, link(3, 1, q[0], h, ahead, send_e.at[h])),
            (has_behind, link(3, 5, q[0], h, behind, send_f.at[h])),
        )

    def swap(h):
        return (valid[5], link(5, 5, q[0], h, partner, send_g.at[h]))

    def arrivals_one(h):
        @pl.when(even)
        def _():
            passed(4, q[1], h, (has_ahead, link(4, 3, q[1], h, across, send_d.at[1, h])))
            passed(3, q[0], h, *onward(h))
            passed(0, q[0], h)

        @pl.when(odd == 1)
        def _():
            passed(0, q[0], h, (has_behind, link(0, 1, q[0], h, across, send_d.at[0, h])))
            passed(4, q[1], h)
            passed(1, q[1], h)

    def arrivals_two(h):
        @pl.when(even)
        def _():
            passed(4, q[0], h, (has_ahead, link(4, 3, q[0], h, across, send_d.at[0, h])))
            passed(3, q[1], h)
            passed(0, q[1], h)

        @pl.when(odd == 1)
        def _():
            passed(3, q[0], h, *onward(h))
            passed(4, q[0], h)
            passed(0, q[1], h)

    def arrivals_three(h):
        passed(5, q[0], h, swap(h))
        passed(1, q[0], h)

        @pl.when(even)
        def _():
            passed(1, q[1], h)

        @pl.when(odd == 1)
        def _():
            passed(3, q[1], h)

    def arrivals_four(h):
        passed(5, q[1], h)
        for slot in (0, 1, 3, 4, 5):

            @pl.when(valid[slot])
            def _(slot=slot):
                for j in range(2):
                    pltpu.make_async_remote_copy(
                        src_ref=rows(slot, 2 * (1 - core) + j, h),
                        dst_ref=rows(slot, 2 * (1 - core) + j, h),
                        send_sem=send_x.at[slot, j, h],
                        recv_sem=recv_x.at[slot, j, h],
                        device_id=sibling,
                        device_id_type=MESH,
                    ).wait_recv()

    def band_weights(block, carry):
        for cc in range(CB):
            for d in range(FIELD):
                taps = weights[block * CB + cc, :, d * TAPS : (d + 1) * TAPS]
                if cc % 2:
                    wide = jnp.concatenate(
                        [taps.astype(jnp.float32), jnp.zeros((MAPS, LEFT), jnp.float32)], axis=1
                    )
                    taps = pltpu.roll(wide, CH, 1).astype(jnp.bfloat16)
                before = (cc // 2) * LEFT
                after = BAND - before - taps.shape[1]
                parts = [taps]
                if before:
                    parts = [jnp.zeros((MAPS, before), jnp.bfloat16)] + parts
                if after:
                    parts = parts + [jnp.zeros((MAPS, after), jnp.bfloat16)]
                banded[block, cc * MAPS : (cc + 1) * MAPS, d * BAND : (d + 1) * BAND] = (
                    jnp.concatenate(parts, axis=1)
                )
        return carry

    def forward(h, low, high):
        at = slice(h * span, (h + 1) * span)

        def one_block(block, carry):
            lanes = pl.multiple_of(block * (CB * CH), CB * CH)
            patches = jnp.concatenate([x[d][at, pl.ds(lanes, BAND)] for d in range(FIELD)], axis=1)
            total = lax.dot_general(
                banded[block], patches, (((1,), (1,)), ((), ())), preferred_element_type=jnp.float32
            )
            active = jnp.tanh(FACTOR * total)
            of_block = pl.ds(pl.multiple_of(block * (CB * MAPS), CB * MAPS), CB * MAPS)
            of_piece = slice(h * piece, (h + 1) * piece)
            wanted = jnp.concatenate(
                [targets[p, of_block, of_piece].astype(jnp.float32) for p in range(POOL)], axis=1
            )
            signal[block] = ((active - wanted) * (1.0 - active * active)).astype(jnp.bfloat16)
            return carry

        lax.fori_loop(low, high, one_block, 0)

    strip = 32

    def select(h):
        def one_strip(i, carry):
            at = pl.ds(pl.multiple_of(i * strip, strip), strip)
            parts = [signal[block, at, :] for block in range(REPS)]
            results = []
            for k in range(REPS):
                taken = None
                for block in range(REPS):
                    scale = jnp.full((strip, span), pick[k][block], jnp.float32)
                    term = scale.astype(jnp.bfloat16) * parts[block]
                    taken = term if taken is None else taken + term
                results.append(taken)
            own[h, at, :] = results[0]
            chosen[h, 0, at, :] = results[1]
            kept[h, at, :] = results[2]
            chosen[h, 1, at, :] = results[3]
            return carry

        lax.fori_loop(0, CB * MAPS // strip, one_strip, 0)
        choice(h).start()

    def choice(h):
        return pltpu.make_async_remote_copy(
            src_ref=chosen.at[h],
            dst_ref=chosen_in.at[h],
            send_sem=send_s.at[h],
            recv_sem=recv_s.at[h],
            device_id=sibling,
            device_id_type=MESH,
        )

    def pair_copy(h):
        return pltpu.make_async_remote_copy(
            src_ref=pair.at[h],
            dst_ref=pair_in.at[h],
            send_sem=send_p.at[h],
            recv_sem=recv_p.at[h],
            device_id=partner,
            device_id_type=MESH,
        )

    def make_pair(h):
        choice(h).wait_recv()

        def one_strip(i, carry):
            at = pl.ds(pl.multiple_of(i * strip, strip), strip)
            pair[h, at, :] = (
                count[0] * kept[h, at, :].astype(jnp.float32)
                + count[1] * chosen_in[h, 1, at, :].astype(jnp.float32)
            ).astype(jnp.bfloat16)
            return carry

        lax.fori_loop(0, CB * MAPS // strip, one_strip, 0)
        pair_copy(h).start()

    def combine(h):
        pair_copy(h).wait_recv()

        def one_strip(i, carry):
            at = pl.ds(pl.multiple_of(i * strip, strip), strip)
            combined[at, h * span : (h + 1) * span] = (
                count[0] * own[h, at, :].astype(jnp.float32)
                + count[1] * chosen_in[h, 0, at, :].astype(jnp.float32)
                + pair_in[h, at, :].astype(jnp.float32)
            ).astype(jnp.bfloat16)
            return carry

        lax.fori_loop(0, CB * MAPS // strip, one_strip, 0)

    def own_window(h):
        def one_strip(i, carry):
            at = pl.ds(pl.multiple_of(h * span + i * strip, strip), strip)
            for d in range(FIELD):
                taken = None
                for block in range(REPS):
                    scale = jnp.full((strip, BAND), pick[0][block], jnp.float32)
                    lanes = slice(block * CB * CH, block * CB * CH + BAND)
                    term = scale.astype(jnp.bfloat16) * x[d][at, lanes]
                    taken = term if taken is None else taken + term
                window[d, at, :] = taken
            return carry

        lax.fori_loop(0, span // strip, one_strip, 0)

    natives()
    loads[0].wait()
    lax.fori_loop(0, REPS, band_weights, 0)
    for load in loads[1:]:
        load.wait()
    for h in range(PIECES):
        arrivals_one(h)
    for h in range(PIECES):
        arrivals_two(h)
    arrivals_three(0)
    for h in range(PIECES):
        if h + 1 < PIECES:
            arrivals_three(h + 1)
        arrivals_four(h)
        forward(h, 0, REPS // 2)
        if h:
            make_pair(h - 1)
        forward(h, REPS // 2, REPS)
        select(h)
        own_window(h)
    make_pair(PIECES - 1)
    for h in range(PIECES):
        combine(h)

    def part_of(ref, d):
        return ref.at[:, :, pl.ds(d * TAPS, TAPS)]

    def send_across(d):
        return pltpu.make_async_remote_copy(
            src_ref=part_of(mine, d),
            dst_ref=part_of(theirs, d),
            send_sem=send_w.at[0, d],
            recv_sem=recv_w.at[0, d],
            device_id=partner,
            device_id_type=MESH,
        )

    def send_beside(d):
        return pltpu.make_async_remote_copy(
            src_ref=part_of(mine, d),
            dst_ref=part_of(fetched_ref.at[1], d),
            send_sem=send_w.at[1, d],
            recv_sem=recv_w.at[1, d],
            device_id=sibling,
            device_id_type=MESH,
        )

    def pass_beside(d):
        return pltpu.make_async_remote_copy(
            src_ref=part_of(theirs, d),
            dst_ref=part_of(fetched_ref.at[3], d),
            send_sem=send_w.at[2, d],
            recv_sem=recv_w.at[2, d],
            device_id=sibling,
            device_id_type=MESH,
        )

    def stores(d):
        return [
            pltpu.make_async_copy(
                part_of(mine, d), part_of(fetched_ref.at[0], d), sem_store.at[0, d]
            ),
            pltpu.make_async_copy(part_of(master, d), part_of(master_out, d), sem_store.at[1, d]),
            pltpu.make_async_copy(part_of(accum, d), part_of(accum_out, d), sem_store.at[2, d]),
        ]

    def store_theirs(d):
        return pltpu.make_async_copy(
            part_of(theirs, d), part_of(fetched_ref.at[2], d), sem_store.at[3, d]
        )

    def send_part(d):
        send_across(d).start()
        send_beside(d).start()
        for store in stores(d):
            store.start()

    for d in range(FIELD):
        for at in range(0, BAND, 256):
            wide = min(256, BAND - at)
            grad[:, at : at + wide] = jnp.dot(
                combined[...],
                window[d, :, at : at + wide],
                preferred_element_type=jnp.float32,
            )
        if d:
            send_part(d - 1)
        for cc in range(CB):
            before = (cc // 2) * LEFT
            of_column = slice(cc * MAPS, (cc + 1) * MAPS)
            if cc % 2:
                wide = grad[of_column, before : before + TAPS + LEFT]
                column = pltpu.roll(wide, TAPS + LEFT - CH, 1)[:, :TAPS]
            else:
                column = grad[of_column, before : before + TAPS]
            slot_grad = FACTOR * column
            taps = slice(d * TAPS, (d + 1) * TAPS)
            accum_next = accum[cc, :, taps] + slot_grad * slot_grad
            master_next = master[cc, :, taps] - LEARNING_RATE * slot_grad / (
                jnp.sqrt(accum_next) + EPSILON
            )
            accum[cc, :, taps] = accum_next
            master[cc, :, taps] = master_next
            mine[cc, :, taps] = master_next.astype(jnp.bfloat16)

    send_part(FIELD - 1)
    for d in range(FIELD):
        send_across(d).wait_recv()
        pass_beside(d).start()
        store_theirs(d).start()

    for d in range(FIELD):
        send_across(d).wait_send()
        send_beside(d).wait()
        for store in stores(d):
            store.wait()
        store_theirs(d).wait()
        pass_beside(d).wait()
    pieces = range(PIECES)
    for h in pieces:
        choice(h).wait_send()
        pair_copy(h).wait_send()

    def all_sent(condition, sems):
        @pl.when(condition)
        def _():
            for sem in sems:
                link(OWN, OWN, 0, 0, partner, sem).wait_send()

    all_sent(has_ahead, [send_a.at[i, h] for i in (0, 1) for h in pieces])
    all_sent(has_behind, [send_b.at[i, h] for i in (0, 1) for h in pieces])
    all_sent(s >= 0, [send_c.at[0, h] for h in pieces])
    all_sent((odd == 1) | (s == 0), [send_c.at[1, h] for h in pieces])
    all_sent((even & has_ahead) | ((odd == 1) & has_behind), [send_d.at[0, h] for h in pieces])
    all_sent(even & has_ahead, [send_d.at[1, h] for h in pieces])
    all_sent(has_ahead, [send_e.at[h] for h in pieces])
    all_sent(has_behind & valid[3], [send_f.at[h] for h in pieces])
    all_sent(valid[5], [send_g.at[h] for h in pieces])
    for slot in (0, 1, 3, 4, 5):
        all_sent(valid[slot], [send_x.at[slot, j, h] for j in (0, 1) for h in pieces])


def place_kernel(
    pieces,
    owner_ref,
    fetched_ref,
    master_ref,
    accum_ref,
    working_out,
    master_out,
    accum_out,
    fetched,
    master,
    accum,
    sem_in,
    sem_out,
):
    g = lax.axis_index("rep")
    columns = CB // pieces
    moves = []
    for block in range(REPS):
        owner = 0
        for i in range(REPS):
            owner = jnp.where(owner_ref[i] == block, i, owner)
        k = 2 * ((owner // 2 + g // 2) % 2) + (owner + g) % 2
        for piece in range(pieces):
            at = pl.ds(block * CB + piece * columns, columns)
            moves.append(
                (
                    fetched_ref.at[k, pl.ds(piece * columns, columns)],
                    fetched.at[at],
                    working_out.at[at],
                )
            )
    for cc in range(CB):
        moves.append((master_ref.at[cc], master.at[cc], master_out.at[cc]))
        moves.append((accum_ref.at[cc], accum.at[cc], accum_out.at[cc]))
    into = [pltpu.make_async_copy(a, b, sem_in.at[i]) for i, (a, b, _) in enumerate(moves)]
    out = [pltpu.make_async_copy(b, c, sem_out.at[i]) for i, (_, b, c) in enumerate(moves)]
    for copy in into:
        copy.start()
    for first, second in zip(into, out):
        first.wait()
        second.start()
    for copy in out:
        copy.wait()


def per_device(
    working, master_slots, accum_slots, pool_images, pool_targets, batch_index, owner_map
):
    sites = lax.axis_size("site")
    batch = pool_images.shape[1]
    width = pool_images.shape[3]
    weights = working[0, 0]
    columns, maps, kdim = weights.shape
    padded = width - CB * CH + BAND
    span = POOL * (batch // PIECES)
    any_space = pl.BlockSpec(memory_space=pl.ANY)
    smem = pl.BlockSpec(memory_space=pltpu.SMEM)
    dma = pltpu.SemaphoreType.DMA
    fetched, master_next, accum_next = pl.pallas_call(
        functools.partial(step_kernel, sites),
        out_shape=(
            jax.ShapeDtypeStruct((REPS, CB, maps, kdim), jnp.bfloat16),
            jax.ShapeDtypeStruct((CB, maps, kdim), jnp.float32),
            jax.ShapeDtypeStruct((CB, maps, kdim), jnp.float32),
        ),
        in_specs=[smem, smem] + [any_space] * 5,
        out_specs=(any_space, any_space, any_space),
        scratch_shapes=[pltpu.VMEM((POOL * batch, padded), jnp.bfloat16)] * FIELD
        + [
            pltpu.VMEM((columns, maps, kdim), jnp.bfloat16),
            pltpu.VMEM((REPS, CB * maps, FIELD * BAND), jnp.bfloat16),
            pltpu.VMEM((POOL, columns * maps, batch), jnp.bfloat16),
            pltpu.VMEM((REPS, CB * maps, span), jnp.bfloat16),
            pltpu.VMEM((PIECES, 2, CB * maps, span), jnp.bfloat16),
            pltpu.VMEM((PIECES, 2, CB * maps, span), jnp.bfloat16),
            pltpu.VMEM((PIECES, CB * maps, span), jnp.bfloat16),
            pltpu.VMEM((PIECES, CB * maps, span), jnp.bfloat16),
            pltpu.VMEM((PIECES, CB * maps, span), jnp.bfloat16),
            pltpu.VMEM((PIECES, CB * maps, span), jnp.bfloat16),
            pltpu.VMEM((CB * maps, POOL * batch), jnp.bfloat16),
            pltpu.VMEM((FIELD, POOL * batch, BAND), jnp.bfloat16),
            pltpu.VMEM((CB, maps, kdim), jnp.float32),
            pltpu.VMEM((CB, maps, kdim), jnp.float32),
            pltpu.VMEM((CB, maps, kdim), jnp.bfloat16),
            pltpu.VMEM((CB, maps, kdim), jnp.bfloat16),
            pltpu.VMEM((CB * maps, BAND), jnp.float32),
            dma((POOL + 4, PIECES)),
            dma((2, PIECES)),
            dma((2, PIECES)),
            dma((2, PIECES)),
            dma((2, PIECES)),
            dma((PIECES,)),
            dma((PIECES,)),
            dma((PIECES,)),
            dma((FIELD, 2, PIECES)),
            dma((FIELD, 2, PIECES)),
            dma((FIELD, 2, PIECES)),
            dma((PIECES,)),
            dma((PIECES,)),
            dma((PIECES,)),
            dma((PIECES,)),
            dma((3, FIELD)),
            dma((3, FIELD)),
            dma((4, FIELD)),
        ],
        compiler_params=pltpu.CompilerParams(
            collective_id=0, has_side_effects=True, vmem_limit_bytes=62 * 1024 * 1024
        ),
        name="step",
    )(
        batch_index,
        owner_map,
        pool_images[:, :, 0, :],
        pool_targets.reshape(POOL, columns * maps, batch),
        weights,
        master_slots[0, 0],
        accum_slots[0, 0],
    )
    pieces = 2
    working_next, master_next, accum_next = pl.pallas_call(
        functools.partial(place_kernel, pieces),
        out_shape=(
            jax.ShapeDtypeStruct((columns, maps, kdim), jnp.bfloat16),
            jax.ShapeDtypeStruct((CB, maps, kdim), jnp.float32),
            jax.ShapeDtypeStruct((CB, maps, kdim), jnp.float32),
        ),
        in_specs=[smem] + [any_space] * 3,
        out_specs=(any_space, any_space, any_space),
        scratch_shapes=[
            pltpu.VMEM((columns, maps, kdim), jnp.bfloat16),
            pltpu.VMEM((CB, maps, kdim), jnp.float32),
            pltpu.VMEM((CB, maps, kdim), jnp.float32),
            dma((REPS * pieces + 2 * CB,)),
            dma((REPS * pieces + 2 * CB,)),
        ],
        compiler_params=pltpu.CompilerParams(vmem_limit_bytes=62 * 1024 * 1024),
        name="place",
    )(owner_map, fetched, master_next, accum_next)
    working_next = working_next[None]
    return (working_next, master_next[None, None], accum_next[None, None])


def solution(mesh):
    placed = (
        P("rep", "site", None, None, None),
        P("site", "rep", None, None, None),
        P("site", "rep", None, None, None),
        P(None, None, "site", None),
        P(None, "site", None, None, None),
        P(),
        P(),
    )
    return jax.shard_map(
        per_device,
        mesh=mesh,
        in_specs=placed,
        out_specs=(
            P("site", None, None, None),
            P("site", "rep", None, None, None),
            P("site", "rep", None, None, None),
        ),
        check_vma=False,
    )
```

```python
import functools

import jax
import jax.numpy as jnp
from jax import lax
from jax.experimental import pallas as pl
from jax.experimental.pallas import tpu as pltpu
from jax.sharding import PartitionSpec as P

MICRO = 3
POOL = 4
FIELD = 6
REPS = 4
CB = 4
CH = 64
MAPS = 64
TAPS = FIELD * CH
BAND = 640
LEFT = 128
PIECES = 4
EARLY = (0, 2, 4)
LATE = (1, 3, 5)
OWN = 2
FACTOR = (FIELD * FIELD * CH) ** (-0.5)
LEARNING_RATE = 0.3
EPSILON = 1e-08

MESH = pl.DeviceIdType.MESH


def step_kernel(
    sites,
    index_ref,
    owner_ref,
    images_ref,
    targets_ref,
    working_ref,
    master_ref,
    accum_ref,
    fetched_ref,
    master_out,
    accum_out,
    x0,
    x1,
    x2,
    x3,
    x4,
    x5,
    weights,
    banded,
    targets,
    signal,
    chosen,
    chosen_in,
    kept,
    own,
    pair,
    pair_in,
    combined,
    window,
    partial,
    grad,
    sem_load,
    send_a,
    send_b,
    send_c,
    send_d,
    send_e,
    send_f,
    send_g,
    send_x,
    recv_l,
    recv_x,
    send_s,
    recv_s,
    send_p,
    recv_p,
    send_w,
    recv_w,
):
    x = [x0, x1, x2, x3, x4, x5]
    batch = images_ref.shape[1]
    width = images_ref.shape[2]
    piece = batch // PIECES
    span = POOL * piece

    g = lax.axis_index("rep")
    s = lax.axis_index("site")
    side = g // 2
    core = g % 2
    odd = s % 2
    even = odd == 0

    def peer(k):
        return 2 * ((side + k // 2) % 2) + (core + k % 2) % 2

    ahead = (g, s + 2)
    behind = (g, s - 2)
    across = (2 * (1 - side) + core, s + 1 - 2 * odd)
    partner = (2 * (1 - side) + core, s)
    sibling = (2 * side + 1 - core, s)
    has_ahead = s + 2 < sites
    has_behind = s >= 2
    valid = [(s + d - 2 >= 0) & (s + d - 2 < sites) for d in range(FIELD)]

    def same(a, b):
        return (1 - jnp.minimum(jnp.abs(a - b), 1)).astype(jnp.float32)

    pick = [[same(owner_ref[peer(k)], block) for block in range(REPS)] for k in range(REPS)]
    entry = lax.broadcasted_iota(jnp.int32, (1, span), 1) // piece
    count = []
    for k in range(2):
        of_lane = jnp.zeros((1, span), jnp.float32)
        for p in range(POOL):
            times = sum(same(index_ref[peer(k), m], p) for m in range(MICRO))
            of_lane = jnp.where(entry == p, times, of_lane)
        count.append(of_lane)

    barrier = pltpu.get_barrier_semaphore()
    for device in (across, partner, sibling):
        pl.semaphore_signal(barrier, inc=1, device_id=device, device_id_type=MESH)

    @pl.when(has_ahead)
    def _():
        pl.semaphore_signal(barrier, inc=1, device_id=ahead, device_id_type=MESH)

    @pl.when(has_behind)
    def _():
        pl.semaphore_signal(barrier, inc=1, device_id=behind, device_id_type=MESH)

    def own_image(p, h):
        return pltpu.make_async_copy(
            images_ref.at[p, pl.ds(h * piece, piece)],
            x[OWN].at[pl.ds(h * span + p * piece, piece), pl.ds(LEFT, width)],
            sem_load.at[p, h],
        )

    loads = [
        pltpu.make_async_copy(working_ref, weights, sem_load.at[POOL, 0]),
        pltpu.make_async_copy(targets_ref, targets, sem_load.at[POOL + 1, 0]),
        pltpu.make_async_copy(master_ref, master_out, sem_load.at[POOL + 2, 0]),
        pltpu.make_async_copy(accum_ref, accum_out, sem_load.at[POOL + 3, 0]),
    ]
    for h in range(PIECES):
        for p in range(POOL):
            own_image(p, h).start()
    for load in loads:
        load.start()

    right = x[0].shape[1] - LEFT - width
    for d in range(FIELD):
        x[d][:, 0:LEFT] = jnp.zeros((POOL * batch, LEFT), jnp.bfloat16)
        x[d][:, LEFT + width :] = jnp.zeros((POOL * batch, right), jnp.bfloat16)
        if d != OWN:

            @pl.when(jnp.logical_not(valid[d]))
            def _(d=d):
                x[d][:, LEFT : LEFT + width] = jnp.zeros((POOL * batch, width), jnp.bfloat16)

    pl.semaphore_wait(barrier, 3 + has_ahead.astype(jnp.int32) + has_behind.astype(jnp.int32))

    q = (2 * core + side, 2 * core + 1 - side)

    def rows(slot, p, h):
        return x[slot].at[
            pl.ds(pl.multiple_of(h * span + p * piece, piece), piece), pl.ds(LEFT, width)
        ]

    def link(src, dst, p, h, device, sem):
        return pltpu.make_async_remote_copy(
            src_ref=rows(src, p, h),
            dst_ref=rows(dst, p, h),
            send_sem=sem,
            recv_sem=recv_l.at[dst, p % 2, h],
            device_id=device,
            device_id_type=MESH,
        )

    def hand_over(slot, p, h):
        return pltpu.make_async_remote_copy(
            src_ref=rows(slot, p, h),
            dst_ref=rows(slot, p, h),
            send_sem=send_x.at[slot, p % 2, h],
            recv_sem=recv_x.at[slot, p % 2, h],
            device_id=sibling,
            device_id_type=MESH,
        )

    def natives():
        for h in range(PIECES):
            for p in range(POOL):
                own_image(p, h).wait()

        @pl.when(has_ahead)
        def _():
            for i in (0, 1):
                for h in range(PIECES):
                    link(OWN, 0, q[i], h, ahead, send_a.at[i, h]).start()

        @pl.when(has_behind)
        def _():
            for i in (1, 0):
                for h in range(PIECES):
                    link(OWN, 4, q[i], h, behind, send_b.at[i, h]).start()

        @pl.when(even)
        def _():
            for h in range(PIECES):
                link(OWN, 1, q[0], h, across, send_c.at[0, h]).start()

        @pl.when(odd == 1)
        def _():
            for i in (1, 0):
                for h in range(PIECES):
                    link(OWN, 3, q[i], h, across, send_c.at[i, h]).start()

    def passed(slot, p, h, *sends):
        @pl.when(valid[slot])
        def _():
            link(slot, slot, p, h, partner, send_a.at[0, 0]).wait_recv()
            for condition, copy in sends:

                @pl.when(condition)
                def _(copy=copy):
                    copy.start()

            hand_over(slot, p, h).start()

    def onward(h):
        return (
            (has_ahead, link(3, 1, q[0], h, ahead, send_e.at[h])),
            (has_behind, link(3, 5, q[0], h, behind, send_f.at[h])),
        )

    def swap(h):
        return (valid[5], link(5, 5, q[0], h, partner, send_g.at[h]))

    def arrivals_one(h):
        @pl.when(even)
        def _():
            passed(4, q[1], h, (has_ahead, link(4, 3, q[1], h, across, send_d.at[1, h])))
            passed(3, q[0], h, *onward(h))
            passed(0, q[0], h)

        @pl.when(odd == 1)
        def _():
            passed(0, q[0], h, (has_behind, link(0, 1, q[0], h, across, send_d.at[0, h])))
            passed(4, q[1], h)
            passed(1, q[1], h, (s == 1, link(1, 1, q[1], h, partner, send_b.at[1, h])))

    def arrivals_two(h):
        @pl.when(even)
        def _():
            passed(4, q[0], h, (has_ahead, link(4, 3, q[0], h, across, send_d.at[0, h])))
            passed(3, q[1], h)
            passed(0, q[1], h)

        @pl.when(odd == 1)
        def _():
            passed(3, q[0], h, *onward(h))
            passed(4, q[0], h)
            passed(0, q[1], h)

    def arrivals_three(h):
        passed(5, q[0], h, swap(h))
        passed(1, q[0], h)

        @pl.when(even)
        def _():
            passed(1, q[1], h)

        @pl.when(odd == 1)
        def _():
            passed(3, q[1], h)

    def arrivals_four(h):
        passed(5, q[1], h)

    def handed(h, slots):
        for slot in slots:

            @pl.when(valid[slot])
            def _(slot=slot):
                for j in range(2):
                    pltpu.make_async_remote_copy(
                        src_ref=rows(slot, 2 * (1 - core) + j, h),
                        dst_ref=rows(slot, 2 * (1 - core) + j, h),
                        send_sem=send_x.at[slot, j, h],
                        recv_sem=recv_x.at[slot, j, h],
                        device_id=sibling,
                        device_id_type=MESH,
                    ).wait_recv()

    def band_weights(block, carry):
        for cc in range(CB):
            for place, d in enumerate(EARLY + LATE):
                taps = weights[block * CB + cc, :, d * TAPS : (d + 1) * TAPS]
                if cc % 2:
                    wide = jnp.concatenate(
                        [taps.astype(jnp.float32), jnp.zeros((MAPS, LEFT), jnp.float32)], axis=1
                    )
                    taps = pltpu.roll(wide, CH, 1).astype(jnp.bfloat16)
                before = (cc // 2) * LEFT
                after = BAND - before - taps.shape[1]
                parts = [taps]
                if before:
                    parts = [jnp.zeros((MAPS, before), jnp.bfloat16)] + parts
                if after:
                    parts = parts + [jnp.zeros((MAPS, after), jnp.bfloat16)]
                banded[block, cc * MAPS : (cc + 1) * MAPS, place * BAND : (place + 1) * BAND] = (
                    jnp.concatenate(parts, axis=1)
                )
        return carry

    half_taps = len(EARLY) * BAND

    def product(h, block, slots, taps):
        at = slice(h * span, (h + 1) * span)
        lanes = pl.multiple_of(block * (CB * CH), CB * CH)
        patches = jnp.concatenate([x[d][at, pl.ds(lanes, BAND)] for d in slots], axis=1)
        return lax.dot_general(
            banded[block, :, taps],
            patches,
            (((1,), (1,)), ((), ())),
            preferred_element_type=jnp.float32,
        )

    def early(h):
        def one_block(block, carry):
            partial[h, block] = product(h, block, EARLY, slice(0, half_taps))
            return carry

        lax.fori_loop(0, REPS, one_block, 0)

    def forward(h, low, high):
        def one_block(block, carry):
            total = partial[h, block] + product(h, block, LATE, slice(half_taps, 2 * half_taps))
            active = jnp.tanh(FACTOR * total)
            of_block = pl.ds(pl.multiple_of(block * (CB * MAPS), CB * MAPS), CB * MAPS)
            of_piece = slice(h * piece, (h + 1) * piece)
            wanted = jnp.concatenate(
                [targets[p, of_block, of_piece].astype(jnp.float32) for p in range(POOL)], axis=1
            )
            signal[block] = ((active - wanted) * (1.0 - active * active)).astype(jnp.bfloat16)
            return carry

        lax.fori_loop(low, high, one_block, 0)

    strip = 32

    def select(h):
        def one_strip(i, carry):
            at = pl.ds(pl.multiple_of(i * strip, strip), strip)
            parts = [signal[block, at, :] for block in range(REPS)]
            results = []
            for k in range(REPS):
                taken = None
                for block in range(REPS):
                    scale = jnp.full((strip, span), pick[k][block], jnp.float32)
                    term = scale.astype(jnp.bfloat16) * parts[block]
                    taken = term if taken is None else taken + term
                results.append(taken)
            own[h, at, :] = results[0]
            chosen[h, 0, at, :] = results[1]
            kept[h, at, :] = results[2]
            chosen[h, 1, at, :] = results[3]
            return carry

        lax.fori_loop(0, CB * MAPS // strip, one_strip, 0)
        choice(h).start()

    def choice(h):
        return pltpu.make_async_remote_copy(
            src_ref=chosen.at[h],
            dst_ref=chosen_in.at[h],
            send_sem=send_s.at[h],
            recv_sem=recv_s.at[h],
            device_id=sibling,
            device_id_type=MESH,
        )

    def pair_copy(h):
        return pltpu.make_async_remote_copy(
            src_ref=pair.at[h],
            dst_ref=pair_in.at[h],
            send_sem=send_p.at[h],
            recv_sem=recv_p.at[h],
            device_id=partner,
            device_id_type=MESH,
        )

    def make_pair(h):
        choice(h).wait_recv()

        def one_strip(i, carry):
            at = pl.ds(pl.multiple_of(i * strip, strip), strip)
            pair[h, at, :] = (
                count[0] * kept[h, at, :].astype(jnp.float32)
                + count[1] * chosen_in[h, 1, at, :].astype(jnp.float32)
            ).astype(jnp.bfloat16)
            return carry

        lax.fori_loop(0, CB * MAPS // strip, one_strip, 0)
        pair_copy(h).start()

    def combine(h):
        pair_copy(h).wait_recv()

        def one_strip(i, carry):
            at = pl.ds(pl.multiple_of(i * strip, strip), strip)
            combined[at, h * span : (h + 1) * span] = (
                count[0] * own[h, at, :].astype(jnp.float32)
                + count[1] * chosen_in[h, 0, at, :].astype(jnp.float32)
                + pair_in[h, at, :].astype(jnp.float32)
            ).astype(jnp.bfloat16)
            return carry

        lax.fori_loop(0, CB * MAPS // strip, one_strip, 0)

    def own_window(h, slots):
        def one_strip(i, carry):
            at = pl.ds(pl.multiple_of(h * span + i * strip, strip), strip)
            for d in slots:
                taken = None
                for block in range(REPS):
                    scale = jnp.full((strip, BAND), pick[0][block], jnp.float32)
                    lanes = slice(block * CB * CH, block * CB * CH + BAND)
                    term = scale.astype(jnp.bfloat16) * x[d][at, lanes]
                    taken = term if taken is None else taken + term
                window[d, at, :] = taken
            return carry

        lax.fori_loop(0, span // strip, one_strip, 0)

    natives()
    loads[0].wait()
    lax.fori_loop(0, REPS, band_weights, 0)
    for load in loads[1:]:
        load.wait()
    for h in range(PIECES):
        arrivals_one(h)
    for h in range(PIECES):
        arrivals_two(h)
    for h in range(PIECES):
        handed(h, (0, 4))
        early(h)
        own_window(h, EARLY)
        arrivals_three(h)
    for h in range(PIECES):
        arrivals_four(h)
        handed(h, LATE)
        forward(h, 0, REPS // 2)
        if h:
            make_pair(h - 1)
        forward(h, REPS // 2, REPS)
        select(h)
        own_window(h, LATE)
    make_pair(PIECES - 1)
    for h in range(PIECES):
        combine(h)

    def part_of(ref, d):
        return ref.at[:, :, pl.ds(d * TAPS, TAPS)]

    def block_copy(source, target, d, device, sems):
        return pltpu.make_async_remote_copy(
            src_ref=part_of(fetched_ref.at[source], d),
            dst_ref=part_of(fetched_ref.at[target], d),
            send_sem=send_w.at[sems, d],
            recv_sem=recv_w.at[sems, d],
            device_id=device,
            device_id_type=MESH,
        )

    def send_across(d):
        return block_copy(0, 2, d, partner, 0)

    def send_beside(d):
        return block_copy(0, 1, d, sibling, 1)

    def pass_beside(d):
        return block_copy(2, 3, d, sibling, 2)

    def send_part(d):
        send_across(d).start()
        send_beside(d).start()

    for d in range(FIELD):
        for at in range(0, BAND, 256):
            wide = min(256, BAND - at)
            grad[:, at : at + wide] = jnp.dot(
                combined[...],
                window[d, :, at : at + wide],
                preferred_element_type=jnp.float32,
            )
        if d:
            send_part(d - 1)
        for cc in range(CB):
            before = (cc // 2) * LEFT
            of_column = slice(cc * MAPS, (cc + 1) * MAPS)
            if cc % 2:
                wide = grad[of_column, before : before + TAPS + LEFT]
                column = pltpu.roll(wide, TAPS + LEFT - CH, 1)[:, :TAPS]
            else:
                column = grad[of_column, before : before + TAPS]
            slot_grad = FACTOR * column
            taps = slice(d * TAPS, (d + 1) * TAPS)
            accum_next = accum_out[cc, :, taps] + slot_grad * slot_grad
            master_next = master_out[cc, :, taps] - LEARNING_RATE * slot_grad / (
                jnp.sqrt(accum_next) + EPSILON
            )
            accum_out[cc, :, taps] = accum_next
            master_out[cc, :, taps] = master_next
            fetched_ref[0, cc, :, taps] = master_next.astype(jnp.bfloat16)

    send_part(FIELD - 1)
    for d in range(FIELD):
        send_across(d).wait_recv()
        pass_beside(d).start()

    for d in range(FIELD):
        send_across(d).wait_send()
        send_beside(d).wait()
        pass_beside(d).wait()
    pieces = range(PIECES)
    for h in pieces:
        choice(h).wait_send()
        pair_copy(h).wait_send()

    def all_sent(condition, sems):
        @pl.when(condition)
        def _():
            for sem in sems:
                link(OWN, OWN, 0, 0, partner, sem).wait_send()

    all_sent(has_ahead, [send_a.at[i, h] for i in (0, 1) for h in pieces])
    all_sent(has_behind, [send_b.at[i, h] for i in (0, 1) for h in pieces])
    all_sent(s >= 0, [send_c.at[0, h] for h in pieces])
    all_sent(odd == 1, [send_c.at[1, h] for h in pieces])
    all_sent(s == 1, [send_b.at[1, h] for h in pieces])
    all_sent((even & has_ahead) | ((odd == 1) & has_behind), [send_d.at[0, h] for h in pieces])
    all_sent(even & has_ahead, [send_d.at[1, h] for h in pieces])
    all_sent(has_ahead, [send_e.at[h] for h in pieces])
    all_sent(has_behind & valid[3], [send_f.at[h] for h in pieces])
    all_sent(valid[5], [send_g.at[h] for h in pieces])
    for slot in (0, 1, 3, 4, 5):
        all_sent(valid[slot], [send_x.at[slot, j, h] for j in (0, 1) for h in pieces])


def place_kernel(
    owner_ref, fetched, master, accum, working_out, master_out, accum_out, sem_out
):
    g = lax.axis_index("rep")
    moves = []
    for block in range(REPS):
        owner = 0
        for i in range(REPS):
            owner = jnp.where(owner_ref[i] == block, i, owner)
        k = 2 * ((owner // 2 + g // 2) % 2) + (owner + g) % 2
        for cc in range(0, CB, 2):
            moves.append(
                (fetched.at[k, pl.ds(cc, 2)], working_out.at[pl.ds(block * CB + cc, 2)])
            )
    for cc in range(CB):
        moves.append((master.at[cc], master_out.at[cc]))
        moves.append((accum.at[cc], accum_out.at[cc]))
    copies = [pltpu.make_async_copy(a, b, sem_out.at[i]) for i, (a, b) in enumerate(moves)]
    for copy in copies:
        copy.start()
    for copy in copies:
        copy.wait()


def per_device(
    working, master_slots, accum_slots, pool_images, pool_targets, batch_index, owner_map
):
    sites = lax.axis_size("site")
    batch = pool_images.shape[1]
    width = pool_images.shape[3]
    weights = working[0, 0]
    columns, maps, kdim = weights.shape
    padded = width - CB * CH + BAND
    span = POOL * (batch // PIECES)
    any_space = pl.BlockSpec(memory_space=pl.ANY)
    smem = pl.BlockSpec(memory_space=pltpu.SMEM)
    vmem = pl.BlockSpec(memory_space=pltpu.VMEM)
    dma = pltpu.SemaphoreType.DMA
    fetched, master_next, accum_next = pl.pallas_call(
        functools.partial(step_kernel, sites),
        out_shape=(
            pltpu.VMEM((REPS, CB, maps, kdim), jnp.bfloat16),
            pltpu.VMEM((CB, maps, kdim), jnp.float32),
            pltpu.VMEM((CB, maps, kdim), jnp.float32),
        ),
        in_specs=[smem, smem] + [any_space] * 5,
        out_specs=(vmem, vmem, vmem),
        scratch_shapes=[pltpu.VMEM((POOL * batch, padded), jnp.bfloat16)] * FIELD
        + [
            pltpu.VMEM((columns, maps, kdim), jnp.bfloat16),
            pltpu.VMEM((REPS, CB * maps, FIELD * BAND), jnp.bfloat16),
            pltpu.VMEM((POOL, columns * maps, batch), jnp.bfloat16),
            pltpu.VMEM((REPS, CB * maps, span), jnp.bfloat16),
            pltpu.VMEM((PIECES, 2, CB * maps, span), jnp.bfloat16),
            pltpu.VMEM((PIECES, 2, CB * maps, span), jnp.bfloat16),
            pltpu.VMEM((PIECES, CB * maps, span), jnp.bfloat16),
            pltpu.VMEM((PIECES, CB * maps, span), jnp.bfloat16),
            pltpu.VMEM((PIECES, CB * maps, span), jnp.bfloat16),
            pltpu.VMEM((PIECES, CB * maps, span), jnp.bfloat16),
            pltpu.VMEM((CB * maps, POOL * batch), jnp.bfloat16),
            pltpu.VMEM((FIELD, POOL * batch, BAND), jnp.bfloat16),
            pltpu.VMEM((PIECES, REPS, CB * maps, span), jnp.float32),
            pltpu.VMEM((CB * maps, BAND), jnp.float32),
            dma((POOL + 4, PIECES)),
            dma((2, PIECES)),
            dma((2, PIECES)),
            dma((2, PIECES)),
            dma((2, PIECES)),
            dma((PIECES,)),
            dma((PIECES,)),
            dma((PIECES,)),
            dma((FIELD, 2, PIECES)),
            dma((FIELD, 2, PIECES)),
            dma((FIELD, 2, PIECES)),
            dma((PIECES,)),
            dma((PIECES,)),
            dma((PIECES,)),
            dma((PIECES,)),
            dma((3, FIELD)),
            dma((3, FIELD)),
        ],
        compiler_params=pltpu.CompilerParams(
            collective_id=0, has_side_effects=True, vmem_limit_bytes=52 * 1024 * 1024
        ),
        name="step",
    )(
        batch_index,
        owner_map,
        pool_images[:, :, 0, :],
        pool_targets.reshape(POOL, columns * maps, batch),
        weights,
        master_slots[0, 0],
        accum_slots[0, 0],
    )
    working_next, master_next, accum_next = pl.pallas_call(
        place_kernel,
        out_shape=(
            jax.ShapeDtypeStruct((columns, maps, kdim), jnp.bfloat16),
            jax.ShapeDtypeStruct((CB, maps, kdim), jnp.float32),
            jax.ShapeDtypeStruct((CB, maps, kdim), jnp.float32),
        ),
        in_specs=[smem, vmem, vmem, vmem],
        out_specs=(any_space, any_space, any_space),
        scratch_shapes=[dma((4 * CB,))],
        compiler_params=pltpu.CompilerParams(vmem_limit_bytes=16 * 1024 * 1024),
        name="place",
    )(owner_map, fetched, master_next, accum_next)
    working_next = working_next[None]
    return (working_next, master_next[None, None], accum_next[None, None])


def solution(mesh):
    placed = (
        P("rep", "site", None, None, None),
        P("site", "rep", None, None, None),
        P("site", "rep", None, None, None),
        P(None, None, "site", None),
        P(None, "site", None, None, None),
        P(),
        P(),
    )
    return jax.shard_map(
        per_device,
        mesh=mesh,
        in_specs=placed,
        out_specs=(
            P("site", None, None, None),
            P("site", "rep", None, None, None),
            P("site", "rep", None, None, None),
        ),
        check_vma=False,
    )
```

```python
import functools

import jax
import jax.numpy as jnp
from jax import lax
from jax.experimental import pallas as pl
from jax.experimental.pallas import tpu as pltpu
from jax.sharding import PartitionSpec as P

MICRO = 3
POOL = 4
FIELD = 6
REPS = 4
CB = 4
CH = 64
MAPS = 64
TAPS = FIELD * CH
BAND = 640
LEFT = 128
PIECES = 4
EARLY = (0, 2, 4)
LATE = (1, 3, 5)
OWN = 2
FACTOR = (FIELD * FIELD * CH) ** (-0.5)
LEARNING_RATE = 0.3
EPSILON = 1e-08

MESH = pl.DeviceIdType.MESH


def step_kernel(
    sites,
    index_ref,
    owner_ref,
    images_ref,
    targets_ref,
    working_ref,
    master_ref,
    accum_ref,
    fetched_ref,
    master_out,
    accum_out,
    x0,
    x1,
    x2,
    x3,
    x4,
    x5,
    weights,
    banded,
    targets,
    signal,
    chosen,
    chosen_in,
    kept,
    own,
    pair,
    pair_in,
    combined,
    window,
    partial,
    wanted,
    grad,
    sem_load,
    send_a,
    send_b,
    send_c,
    send_d,
    send_e,
    send_f,
    send_g,
    send_x,
    recv_l,
    recv_x,
    send_s,
    recv_s,
    send_p,
    recv_p,
    send_w,
    recv_w,
):
    x = [x0, x1, x2, x3, x4, x5]
    batch = images_ref.shape[1]
    width = images_ref.shape[2]
    piece = batch // PIECES
    span = POOL * piece

    g = lax.axis_index("rep")
    s = lax.axis_index("site")
    side = g // 2
    core = g % 2
    odd = s % 2
    even = odd == 0

    def peer(k):
        return 2 * ((side + k // 2) % 2) + (core + k % 2) % 2

    ahead = (g, s + 2)
    behind = (g, s - 2)
    across = (2 * (1 - side) + core, s + 1 - 2 * odd)
    partner = (2 * (1 - side) + core, s)
    sibling = (2 * side + 1 - core, s)
    has_ahead = s + 2 < sites
    has_behind = s >= 2
    valid = [(s + d - 2 >= 0) & (s + d - 2 < sites) for d in range(FIELD)]

    def same(a, b):
        return (1 - jnp.minimum(jnp.abs(a - b), 1)).astype(jnp.float32)

    pick = [[same(owner_ref[peer(k)], block) for block in range(REPS)] for k in range(REPS)]
    entry = lax.broadcasted_iota(jnp.int32, (1, span), 1) // piece
    count = []
    for k in range(2):
        of_lane = jnp.zeros((1, span), jnp.float32)
        for p in range(POOL):
            times = sum(same(index_ref[peer(k), m], p) for m in range(MICRO))
            of_lane = jnp.where(entry == p, times, of_lane)
        count.append(of_lane)

    barrier = pltpu.get_barrier_semaphore()
    for device in (across, partner, sibling):
        pl.semaphore_signal(barrier, inc=1, device_id=device, device_id_type=MESH)

    @pl.when(has_ahead)
    def _():
        pl.semaphore_signal(barrier, inc=1, device_id=ahead, device_id_type=MESH)

    @pl.when(has_behind)
    def _():
        pl.semaphore_signal(barrier, inc=1, device_id=behind, device_id_type=MESH)

    def own_image(p, h):
        return pltpu.make_async_copy(
            images_ref.at[p, pl.ds(h * piece, piece)],
            x[OWN].at[pl.ds(h * span + p * piece, piece), pl.ds(LEFT, width)],
            sem_load.at[p, h],
        )

    loads = [
        pltpu.make_async_copy(working_ref, weights, sem_load.at[POOL, 0]),
        pltpu.make_async_copy(targets_ref, targets, sem_load.at[POOL + 1, 0]),
        pltpu.make_async_copy(master_ref, master_out, sem_load.at[POOL + 2, 0]),
        pltpu.make_async_copy(accum_ref, accum_out, sem_load.at[POOL + 3, 0]),
    ]
    for h in range(PIECES):
        for p in range(POOL):
            own_image(p, h).start()
    for load in loads:
        load.start()

    right = x[0].shape[1] - LEFT - width
    for d in range(FIELD):
        x[d][:, 0:LEFT] = jnp.zeros((POOL * batch, LEFT), jnp.bfloat16)
        x[d][:, LEFT + width :] = jnp.zeros((POOL * batch, right), jnp.bfloat16)
        if d != OWN:

            @pl.when(jnp.logical_not(valid[d]))
            def _(d=d):
                x[d][:, LEFT : LEFT + width] = jnp.zeros((POOL * batch, width), jnp.bfloat16)

    pl.semaphore_wait(barrier, 3 + has_ahead.astype(jnp.int32) + has_behind.astype(jnp.int32))

    q = (2 * core + side, 2 * core + 1 - side)

    def rows(slot, p, h):
        return x[slot].at[
            pl.ds(pl.multiple_of(h * span + p * piece, piece), piece), pl.ds(LEFT, width)
        ]

    def link(src, dst, p, h, device, sem):
        return pltpu.make_async_remote_copy(
            src_ref=rows(src, p, h),
            dst_ref=rows(dst, p, h),
            send_sem=sem,
            recv_sem=recv_l.at[dst, p % 2, h],
            device_id=device,
            device_id_type=MESH,
        )

    def hand_over(slot, p, h):
        return pltpu.make_async_remote_copy(
            src_ref=rows(slot, p, h),
            dst_ref=rows(slot, p, h),
            send_sem=send_x.at[slot, p % 2, h],
            recv_sem=recv_x.at[slot, p % 2, h],
            device_id=sibling,
            device_id_type=MESH,
        )

    def natives(h):
        for p in range(POOL):
            own_image(p, h).wait()

        @pl.when(has_ahead)
        def _():
            for i in (0, 1):
                link(OWN, 0, q[i], h, ahead, send_a.at[i, h]).start()

        @pl.when(has_behind)
        def _():
            link(OWN, 4, q[1], h, behind, send_b.at[1, h]).start()

        @pl.when(even)
        def _():
            link(OWN, 1, q[0], h, across, send_c.at[0, h]).start()

        @pl.when(odd == 1)
        def _():
            for i in (1, 0):
                link(OWN, 3, q[i], h, across, send_c.at[i, h]).start()

    def passed(slot, p, h, *sends):
        @pl.when(valid[slot])
        def _():
            link(slot, slot, p, h, partner, send_a.at[0, 0]).wait_recv()
            for condition, copy in sends:

                @pl.when(condition)
                def _(copy=copy):
                    copy.start()

            hand_over(slot, p, h).start()

    def onward(i, h):
        behind_copy = (has_behind, link(3, 5, q[i], h, behind, send_f.at[i, h]))
        if i:
            return (behind_copy,)
        return (has_ahead, link(3, 1, q[0], h, ahead, send_e.at[h])), behind_copy

    def below_first(h):
        swap = (s >= 0, link(4, 4, q[1], h, partner, send_g.at[h]))

        @pl.when(even)
        def _():
            passed(4, q[1], h, swap, (has_ahead, link(4, 3, q[1], h, across, send_d.at[1, h])))

        @pl.when(odd == 1)
        def _():
            passed(4, q[1], h, swap)
            passed(1, q[1], h, (s == 1, link(1, 1, q[1], h, partner, send_b.at[0, h])))

    def below_second(h):
        @pl.when(even)
        def _():
            passed(4, q[0], h, (has_ahead, link(4, 3, q[0], h, across, send_d.at[0, h])))

        @pl.when(odd == 1)
        def _():
            passed(4, q[0], h)

    def straight(h):
        @pl.when(even)
        def _():
            passed(3, q[0], h, *onward(0, h))
            passed(0, q[0], h)
            passed(3, q[1], h, *onward(1, h))

        @pl.when(odd == 1)
        def _():
            passed(0, q[0], h, (has_behind, link(0, 1, q[0], h, across, send_d.at[0, h])))

        passed(0, q[1], h)

    def crossed(i, h):
        @pl.when(odd == 1)
        def _():
            passed(3, q[i], h, *onward(i, h))

    def last_rows(h):
        passed(5, q[0], h)
        passed(1, q[0], h)

        @pl.when(even)
        def _():
            passed(1, q[1], h)

        passed(5, q[1], h)
        handed(h, LATE)

    def handed(h, slots):
        for slot in slots:

            @pl.when(valid[slot])
            def _(slot=slot):
                for j in range(2):
                    pltpu.make_async_remote_copy(
                        src_ref=rows(slot, 2 * (1 - core) + j, h),
                        dst_ref=rows(slot, 2 * (1 - core) + j, h),
                        send_sem=send_x.at[slot, j, h],
                        recv_sem=recv_x.at[slot, j, h],
                        device_id=sibling,
                        device_id_type=MESH,
                    ).wait_recv()

    def band_weights(block, carry):
        for cc in range(CB):
            for place, d in enumerate(EARLY + LATE):
                taps = weights[block * CB + cc, :, d * TAPS : (d + 1) * TAPS]
                if cc % 2:
                    wide = jnp.concatenate(
                        [taps.astype(jnp.float32), jnp.zeros((MAPS, LEFT), jnp.float32)], axis=1
                    )
                    taps = pltpu.roll(wide, CH, 1).astype(jnp.bfloat16)
                before = (cc // 2) * LEFT
                after = BAND - before - taps.shape[1]
                parts = [taps]
                if before:
                    parts = [jnp.zeros((MAPS, before), jnp.bfloat16)] + parts
                if after:
                    parts = parts + [jnp.zeros((MAPS, after), jnp.bfloat16)]
                banded[block, cc * MAPS : (cc + 1) * MAPS, place * BAND : (place + 1) * BAND] = (
                    jnp.concatenate(parts, axis=1)
                )
        return carry

    half_taps = len(EARLY) * BAND

    def product(h, block, slots, taps):
        at = slice(h * span, (h + 1) * span)
        lanes = pl.multiple_of(block * (CB * CH), CB * CH)
        patches = jnp.concatenate([x[d][at, pl.ds(lanes, BAND)] for d in slots], axis=1)
        return lax.dot_general(
            banded[block, :, taps],
            patches,
            (((1,), (1,)), ((), ())),
            preferred_element_type=jnp.float32,
        )

    def early(h):
        handed(h, (0, 4))

        def one_block(block, carry):
            partial[h, block] = product(h, block, EARLY, slice(0, half_taps))
            of_block = pl.ds(pl.multiple_of(block * (CB * MAPS), CB * MAPS), CB * MAPS)
            of_piece = slice(h * piece, (h + 1) * piece)
            wanted[h, of_block, :] = jnp.concatenate(
                [targets[p, of_block, of_piece].astype(jnp.float32) for p in range(POOL)], axis=1
            ).astype(jnp.bfloat16)
            return carry

        lax.fori_loop(0, REPS, one_block, 0)
        own_window(h, EARLY)

    def forward(h, low, high):
        def one_block(block, carry):
            total = partial[h, block] + product(h, block, LATE, slice(half_taps, 2 * half_taps))
            active = jnp.tanh(FACTOR * total)
            of_block = pl.ds(pl.multiple_of(block * (CB * MAPS), CB * MAPS), CB * MAPS)
            gap = active - wanted[h, of_block, :].astype(jnp.float32)
            signal[block] = (gap * (1.0 - active * active)).astype(jnp.bfloat16)
            return carry

        lax.fori_loop(low, high, one_block, 0)

    strip = 32

    def select(h):
        def one_strip(i, carry):
            at = pl.ds(pl.multiple_of(i * strip, strip), strip)
            parts = [signal[block, at, :] for block in range(REPS)]
            results = []
            for k in range(REPS):
                taken = None
                for block in range(REPS):
                    scale = jnp.full((strip, span), pick[k][block], jnp.float32)
                    term = scale.astype(jnp.bfloat16) * parts[block]
                    taken = term if taken is None else taken + term
                results.append(taken)
            own[h, at, :] = results[0]
            chosen[h, 0, at, :] = results[1]
            kept[h, at, :] = results[2]
            chosen[h, 1, at, :] = results[3]
            return carry

        lax.fori_loop(0, CB * MAPS // strip, one_strip, 0)
        choice(h).start()

    def choice(h):
        return pltpu.make_async_remote_copy(
            src_ref=chosen.at[h],
            dst_ref=chosen_in.at[h],
            send_sem=send_s.at[h],
            recv_sem=recv_s.at[h],
            device_id=sibling,
            device_id_type=MESH,
        )

    def pair_copy(h):
        return pltpu.make_async_remote_copy(
            src_ref=pair.at[h],
            dst_ref=pair_in.at[h],
            send_sem=send_p.at[h],
            recv_sem=recv_p.at[h],
            device_id=partner,
            device_id_type=MESH,
        )

    def make_pair(h):
        choice(h).wait_recv()

        def one_strip(i, carry):
            at = pl.ds(pl.multiple_of(i * strip, strip), strip)
            pair[h, at, :] = (
                count[0] * kept[h, at, :].astype(jnp.float32)
                + count[1] * chosen_in[h, 1, at, :].astype(jnp.float32)
            ).astype(jnp.bfloat16)
            return carry

        lax.fori_loop(0, CB * MAPS // strip, one_strip, 0)
        pair_copy(h).start()

    def combine(h):
        pair_copy(h).wait_recv()

        def one_strip(i, carry):
            at = pl.ds(pl.multiple_of(i * strip, strip), strip)
            combined[at, h * span : (h + 1) * span] = (
                count[0] * own[h, at, :].astype(jnp.float32)
                + count[1] * chosen_in[h, 0, at, :].astype(jnp.float32)
                + pair_in[h, at, :].astype(jnp.float32)
            ).astype(jnp.bfloat16)
            return carry

        lax.fori_loop(0, CB * MAPS // strip, one_strip, 0)

    def own_window(h, slots):
        def one_strip(i, carry):
            at = pl.ds(pl.multiple_of(h * span + i * strip, strip), strip)
            for d in slots:
                taken = None
                for block in range(REPS):
                    scale = jnp.full((strip, BAND), pick[0][block], jnp.float32)
                    lanes = slice(block * CB * CH, block * CB * CH + BAND)
                    term = scale.astype(jnp.bfloat16) * x[d][at, lanes]
                    taken = term if taken is None else taken + term
                window[d, at, :] = taken
            return carry

        lax.fori_loop(0, span // strip, one_strip, 0)

    def finish(h):
        last_rows(h)
        forward(h, 0, REPS // 2)
        if h:
            make_pair(h - 1)
        forward(h, REPS // 2, REPS)
        select(h)
        own_window(h, LATE)

    for h in range(PIECES):
        natives(h)
    loads[0].wait()
    lax.fori_loop(0, REPS, band_weights, 0)
    for load in loads[1:]:
        load.wait()
    below_first(0)
    below_first(1)
    straight(0)
    below_second(0)
    below_first(2)
    below_second(1)
    below_first(3)
    straight(1)
    below_second(2)
    below_second(3)
    early(0)
    crossed(0, 0)
    crossed(0, 1)
    straight(2)
    early(1)
    crossed(1, 0)
    crossed(0, 2)
    straight(3)
    early(2)
    crossed(1, 1)
    early(3)
    crossed(0, 3)
    finish(0)
    crossed(1, 2)
    finish(1)
    crossed(1, 3)
    finish(2)
    finish(3)
    make_pair(PIECES - 1)
    for h in range(PIECES):
        combine(h)

    def part_of(ref, d):
        return ref.at[:, :, pl.ds(d * TAPS, TAPS)]

    def block_copy(source, target, d, device, sems):
        return pltpu.make_async_remote_copy(
            src_ref=part_of(fetched_ref.at[source], d),
            dst_ref=part_of(fetched_ref.at[target], d),
            send_sem=send_w.at[sems, d],
            recv_sem=recv_w.at[sems, d],
            device_id=device,
            device_id_type=MESH,
        )

    def send_across(d):
        return block_copy(0, 2, d, partner, 0)

    def send_beside(d):
        return block_copy(0, 1, d, sibling, 1)

    def pass_beside(d):
        return block_copy(2, 3, d, sibling, 2)

    def send_part(d):
        send_across(d).start()
        send_beside(d).start()

    for d in range(FIELD):
        for at in range(0, BAND, 256):
            wide = min(256, BAND - at)
            grad[:, at : at + wide] = jnp.dot(
                combined[...],
                window[d, :, at : at + wide],
                preferred_element_type=jnp.float32,
            )
        if d:
            send_part(d - 1)
        for cc in range(CB):
            before = (cc // 2) * LEFT
            of_column = slice(cc * MAPS, (cc + 1) * MAPS)
            if cc % 2:
                wide = grad[of_column, before : before + TAPS + LEFT]
                column = pltpu.roll(wide, TAPS + LEFT - CH, 1)[:, :TAPS]
            else:
                column = grad[of_column, before : before + TAPS]
            slot_grad = FACTOR * column
            taps = slice(d * TAPS, (d + 1) * TAPS)
            accum_next = accum_out[cc, :, taps] + slot_grad * slot_grad
            master_next = master_out[cc, :, taps] - LEARNING_RATE * slot_grad / (
                jnp.sqrt(accum_next) + EPSILON
            )
            accum_out[cc, :, taps] = accum_next
            master_out[cc, :, taps] = master_next
            fetched_ref[0, cc, :, taps] = master_next.astype(jnp.bfloat16)

    send_part(FIELD - 1)
    for d in range(FIELD):
        send_across(d).wait_recv()
        pass_beside(d).start()

    for d in range(FIELD):
        send_across(d).wait_send()
        send_beside(d).wait()
        pass_beside(d).wait()
    pieces = range(PIECES)
    for h in pieces:
        choice(h).wait_send()
        pair_copy(h).wait_send()

    def all_sent(condition, sems):
        @pl.when(condition)
        def _():
            for sem in sems:
                link(OWN, OWN, 0, 0, partner, sem).wait_send()

    all_sent(has_ahead, [send_a.at[i, h] for i in (0, 1) for h in pieces])
    all_sent(has_behind, [send_b.at[1, h] for h in pieces])
    all_sent(s >= 0, [send_c.at[0, h] for h in pieces])
    all_sent(odd == 1, [send_c.at[1, h] for h in pieces])
    all_sent(s == 1, [send_b.at[0, h] for h in pieces])
    all_sent((even & has_ahead) | ((odd == 1) & has_behind), [send_d.at[0, h] for h in pieces])
    all_sent(even & has_ahead, [send_d.at[1, h] for h in pieces])
    all_sent(has_ahead, [send_e.at[h] for h in pieces])
    all_sent(has_behind & valid[3], [send_f.at[i, h] for i in (0, 1) for h in pieces])
    all_sent(valid[4], [send_g.at[h] for h in pieces])
    for slot in (0, 1, 3, 4, 5):
        all_sent(valid[slot], [send_x.at[slot, j, h] for j in (0, 1) for h in pieces])


def place_kernel(
    owner_ref, fetched, master, accum, working_out, master_out, accum_out, sem_out
):
    g = lax.axis_index("rep")
    moves = []
    for block in range(REPS):
        owner = 0
        for i in range(REPS):
            owner = jnp.where(owner_ref[i] == block, i, owner)
        k = 2 * ((owner // 2 + g // 2) % 2) + (owner + g) % 2
        for cc in range(0, CB, 2):
            moves.append(
                (fetched.at[k, pl.ds(cc, 2)], working_out.at[pl.ds(block * CB + cc, 2)])
            )
    for cc in range(CB):
        moves.append((master.at[cc], master_out.at[cc]))
        moves.append((accum.at[cc], accum_out.at[cc]))
    copies = [pltpu.make_async_copy(a, b, sem_out.at[i]) for i, (a, b) in enumerate(moves)]
    for copy in copies:
        copy.start()
    for copy in copies:
        copy.wait()


def per_device(
    working, master_slots, accum_slots, pool_images, pool_targets, batch_index, owner_map
):
    sites = lax.axis_size("site")
    batch = pool_images.shape[1]
    width = pool_images.shape[3]
    weights = working[0, 0]
    columns, maps, kdim = weights.shape
    padded = width - CB * CH + BAND
    span = POOL * (batch // PIECES)
    any_space = pl.BlockSpec(memory_space=pl.ANY)
    smem = pl.BlockSpec(memory_space=pltpu.SMEM)
    vmem = pl.BlockSpec(memory_space=pltpu.VMEM)
    dma = pltpu.SemaphoreType.DMA
    fetched, master_next, accum_next = pl.pallas_call(
        functools.partial(step_kernel, sites),
        out_shape=(
            pltpu.VMEM((REPS, CB, maps, kdim), jnp.bfloat16),
            pltpu.VMEM((CB, maps, kdim), jnp.float32),
            pltpu.VMEM((CB, maps, kdim), jnp.float32),
        ),
        in_specs=[smem, smem] + [any_space] * 5,
        out_specs=(vmem, vmem, vmem),
        scratch_shapes=[pltpu.VMEM((POOL * batch, padded), jnp.bfloat16)] * FIELD
        + [
            pltpu.VMEM((columns, maps, kdim), jnp.bfloat16),
            pltpu.VMEM((REPS, CB * maps, FIELD * BAND), jnp.bfloat16),
            pltpu.VMEM((POOL, columns * maps, batch), jnp.bfloat16),
            pltpu.VMEM((REPS, CB * maps, span), jnp.bfloat16),
            pltpu.VMEM((PIECES, 2, CB * maps, span), jnp.bfloat16),
            pltpu.VMEM((PIECES, 2, CB * maps, span), jnp.bfloat16),
            pltpu.VMEM((PIECES, CB * maps, span), jnp.bfloat16),
            pltpu.VMEM((PIECES, CB * maps, span), jnp.bfloat16),
            pltpu.VMEM((PIECES, CB * maps, span), jnp.bfloat16),
            pltpu.VMEM((PIECES, CB * maps, span), jnp.bfloat16),
            pltpu.VMEM((CB * maps, POOL * batch), jnp.bfloat16),
            pltpu.VMEM((FIELD, POOL * batch, BAND), jnp.bfloat16),
            pltpu.VMEM((PIECES, REPS, CB * maps, span), jnp.float32),
            pltpu.VMEM((PIECES, columns * maps, span), jnp.bfloat16),
            pltpu.VMEM((CB * maps, BAND), jnp.float32),
            dma((POOL + 4, PIECES)),
            dma((2, PIECES)),
            dma((2, PIECES)),
            dma((2, PIECES)),
            dma((2, PIECES)),
            dma((PIECES,)),
            dma((2, PIECES)),
            dma((PIECES,)),
            dma((FIELD, 2, PIECES)),
            dma((FIELD, 2, PIECES)),
            dma((FIELD, 2, PIECES)),
            dma((PIECES,)),
            dma((PIECES,)),
            dma((PIECES,)),
            dma((PIECES,)),
            dma((3, FIELD)),
            dma((3, FIELD)),
        ],
        compiler_params=pltpu.CompilerParams(
            collective_id=0, has_side_effects=True, vmem_limit_bytes=52 * 1024 * 1024
        ),
        name="step",
    )(
        batch_index,
        owner_map,
        pool_images[:, :, 0, :],
        pool_targets.reshape(POOL, columns * maps, batch),
        weights,
        master_slots[0, 0],
        accum_slots[0, 0],
    )
    working_next, master_next, accum_next = pl.pallas_call(
        place_kernel,
        out_shape=(
            jax.ShapeDtypeStruct((columns, maps, kdim), jnp.bfloat16),
            jax.ShapeDtypeStruct((CB, maps, kdim), jnp.float32),
            jax.ShapeDtypeStruct((CB, maps, kdim), jnp.float32),
        ),
        in_specs=[smem, vmem, vmem, vmem],
        out_specs=(any_space, any_space, any_space),
        scratch_shapes=[dma((4 * CB,))],
        compiler_params=pltpu.CompilerParams(vmem_limit_bytes=16 * 1024 * 1024),
        name="place",
    )(owner_map, fetched, master_next, accum_next)
    working_next = working_next[None]
    return (working_next, master_next[None, None], accum_next[None, None])


def solution(mesh):
    placed = (
        P("rep", "site", None, None, None),
        P("site", "rep", None, None, None),
        P("site", "rep", None, None, None),
        P(None, None, "site", None),
        P(None, "site", None, None, None),
        P(),
        P(),
    )
    return jax.shard_map(
        per_device,
        mesh=mesh,
        in_specs=placed,
        out_specs=(
            P("site", None, None, None),
            P("site", "rep", None, None, None),
            P("site", "rep", None, None, None),
        ),
        check_vma=False,
    )
```

```python
import functools

import jax
import jax.numpy as jnp
from jax import lax
from jax.experimental import pallas as pl
from jax.experimental.pallas import tpu as pltpu
from jax.sharding import PartitionSpec as P

MICRO = 3
POOL = 4
FIELD = 6
REPS = 4
CB = 4
CH = 64
MAPS = 64
TAPS = FIELD * CH
BAND = 640
LEFT = 128
PIECES = 4
EARLY = (0, 2, 4)
LATE = (1, 3, 5)
OWN = 2
FACTOR = (FIELD * FIELD * CH) ** (-0.5)
LEARNING_RATE = 0.3
EPSILON = 1e-08

MESH = pl.DeviceIdType.MESH


def step_kernel(
    sites,
    index_ref,
    owner_ref,
    images_ref,
    targets_ref,
    working_ref,
    master_ref,
    accum_ref,
    fetched_ref,
    master_out,
    accum_out,
    x0,
    x1,
    x2,
    x3,
    x4,
    x5,
    weights,
    banded,
    targets,
    signal,
    chosen,
    chosen_in,
    kept,
    own,
    pair,
    pair_in,
    combined,
    window,
    partial,
    wanted,
    grad,
    sem_load,
    send_a,
    send_b,
    send_c,
    send_d,
    send_e,
    send_f,
    send_g,
    send_x,
    recv_l,
    recv_x,
    send_s,
    recv_s,
    send_p,
    recv_p,
    send_w,
    recv_w,
):
    x = [x0, x1, x2, x3, x4, x5]
    batch = images_ref.shape[1]
    width = images_ref.shape[2]
    piece = batch // PIECES
    span = POOL * piece

    g = lax.axis_index("rep")
    s = lax.axis_index("site")
    side = g // 2
    core = g % 2
    odd = s % 2
    even = odd == 0

    def peer(k):
        return 2 * ((side + k // 2) % 2) + (core + k % 2) % 2

    ahead = (g, s + 2)
    behind = (g, s - 2)
    across = (2 * (1 - side) + core, s + 1 - 2 * odd)
    partner = (2 * (1 - side) + core, s)
    sibling = (2 * side + 1 - core, s)
    has_ahead = s + 2 < sites
    has_behind = s >= 2
    valid = [(s + d - 2 >= 0) & (s + d - 2 < sites) for d in range(FIELD)]

    def same(a, b):
        return (1 - jnp.minimum(jnp.abs(a - b), 1)).astype(jnp.float32)

    pick = [[same(owner_ref[peer(k)], block) for block in range(REPS)] for k in range(REPS)]
    entry = lax.broadcasted_iota(jnp.int32, (1, span), 1) // piece
    count = []
    for k in range(2):
        of_lane = jnp.zeros((1, span), jnp.float32)
        for p in range(POOL):
            times = sum(same(index_ref[peer(k), m], p) for m in range(MICRO))
            of_lane = jnp.where(entry == p, times, of_lane)
        count.append(of_lane)

    barrier = pltpu.get_barrier_semaphore()
    for device in (across, partner, sibling):
        pl.semaphore_signal(barrier, inc=1, device_id=device, device_id_type=MESH)

    @pl.when(has_ahead)
    def _():
        pl.semaphore_signal(barrier, inc=1, device_id=ahead, device_id_type=MESH)

    @pl.when(has_behind)
    def _():
        pl.semaphore_signal(barrier, inc=1, device_id=behind, device_id_type=MESH)

    def own_image(p, h):
        return pltpu.make_async_copy(
            images_ref.at[p, pl.ds(h * piece, piece)],
            x[OWN].at[pl.ds(h * span + p * piece, piece), pl.ds(LEFT, width)],
            sem_load.at[p, h],
        )

    loads = [
        pltpu.make_async_copy(working_ref, weights, sem_load.at[POOL, 0]),
        pltpu.make_async_copy(targets_ref, targets, sem_load.at[POOL + 1, 0]),
        pltpu.make_async_copy(master_ref, master_out, sem_load.at[POOL + 2, 0]),
        pltpu.make_async_copy(accum_ref, accum_out, sem_load.at[POOL + 3, 0]),
    ]
    for h in range(PIECES):
        for p in range(POOL):
            own_image(p, h).start()
    for load in loads:
        load.start()

    right = x[0].shape[1] - LEFT - width
    for d in range(FIELD):
        x[d][:, 0:LEFT] = jnp.zeros((POOL * batch, LEFT), jnp.bfloat16)
        x[d][:, LEFT + width :] = jnp.zeros((POOL * batch, right), jnp.bfloat16)
        if d != OWN:

            @pl.when(jnp.logical_not(valid[d]))
            def _(d=d):
                x[d][:, LEFT : LEFT + width] = jnp.zeros((POOL * batch, width), jnp.bfloat16)

    pl.semaphore_wait(barrier, 3 + has_ahead.astype(jnp.int32) + has_behind.astype(jnp.int32))

    q = (2 * core + side, 2 * core + 1 - side)

    def rows(slot, p, h):
        return x[slot].at[
            pl.ds(pl.multiple_of(h * span + p * piece, piece), piece), pl.ds(LEFT, width)
        ]

    def link(src, dst, p, h, device, sem):
        return pltpu.make_async_remote_copy(
            src_ref=rows(src, p, h),
            dst_ref=rows(dst, p, h),
            send_sem=sem,
            recv_sem=recv_l.at[dst, p % 2, h],
            device_id=device,
            device_id_type=MESH,
        )

    def hand_over(slot, p, h):
        return pltpu.make_async_remote_copy(
            src_ref=rows(slot, p, h),
            dst_ref=rows(slot, p, h),
            send_sem=send_x.at[slot, p % 2, h],
            recv_sem=recv_x.at[slot, p % 2, h],
            device_id=sibling,
            device_id_type=MESH,
        )

    def natives(h):
        for p in range(POOL):
            own_image(p, h).wait()

        @pl.when(has_ahead)
        def _():
            for i in (0, 1):
                link(OWN, 0, q[i], h, ahead, send_a.at[i, h]).start()

        @pl.when(has_behind)
        def _():
            link(OWN, 4, q[1], h, behind, send_b.at[1, h]).start()

        @pl.when(even)
        def _():
            link(OWN, 1, q[0], h, across, send_c.at[0, h]).start()

        @pl.when(odd == 1)
        def _():
            for i in (1, 0):
                link(OWN, 3, q[i], h, across, send_c.at[i, h]).start()

    def passed(slot, p, h, *sends):
        @pl.when(valid[slot])
        def _():
            link(slot, slot, p, h, partner, send_a.at[0, 0]).wait_recv()
            for condition, copy in sends:

                @pl.when(condition)
                def _(copy=copy):
                    copy.start()

            hand_over(slot, p, h).start()

    def onward(i, h):
        behind_copy = (has_behind, link(3, 5, q[i], h, behind, send_f.at[i, h]))
        if i:
            return (behind_copy,)
        return (has_ahead, link(3, 1, q[0], h, ahead, send_e.at[h])), behind_copy

    def below_first(h):
        swap = (s >= 0, link(4, 4, q[1], h, partner, send_g.at[h]))

        @pl.when(even)
        def _():
            passed(4, q[1], h, swap, (has_ahead, link(4, 3, q[1], h, across, send_d.at[1, h])))

        @pl.when(odd == 1)
        def _():
            passed(4, q[1], h, swap)

    def above(h):
        @pl.when(odd == 1)
        def _():
            passed(1, q[1], h, (s == 1, link(1, 1, q[1], h, partner, send_b.at[0, h])))

    def below_second(h):
        @pl.when(even)
        def _():
            passed(4, q[0], h, (has_ahead, link(4, 3, q[0], h, across, send_d.at[0, h])))

        @pl.when(odd == 1)
        def _():
            passed(4, q[0], h)

    def straight(h):
        @pl.when(even)
        def _():
            passed(3, q[0], h, *onward(0, h))
            passed(0, q[0], h)
            passed(3, q[1], h, *onward(1, h))

        @pl.when(odd == 1)
        def _():
            passed(0, q[0], h, (has_behind, link(0, 1, q[0], h, across, send_d.at[0, h])))

        passed(0, q[1], h)

    def crossed(i, h):
        @pl.when(odd == 1)
        def _():
            passed(3, q[i], h, *onward(i, h))

    def last_rows(h):
        passed(5, q[0], h)
        passed(1, q[0], h)

        @pl.when(even)
        def _():
            passed(1, q[1], h)

        passed(5, q[1], h)
        handed(h, LATE)

    def handed(h, slots):
        for slot in slots:

            @pl.when(valid[slot])
            def _(slot=slot):
                for j in range(2):
                    pltpu.make_async_remote_copy(
                        src_ref=rows(slot, 2 * (1 - core) + j, h),
                        dst_ref=rows(slot, 2 * (1 - core) + j, h),
                        send_sem=send_x.at[slot, j, h],
                        recv_sem=recv_x.at[slot, j, h],
                        device_id=sibling,
                        device_id_type=MESH,
                    ).wait_recv()

    def band_weights(block, carry):
        for cc in range(CB):
            for place, d in enumerate(EARLY + LATE):
                taps = weights[block * CB + cc, :, d * TAPS : (d + 1) * TAPS]
                if cc % 2:
                    wide = jnp.concatenate(
                        [taps.astype(jnp.float32), jnp.zeros((MAPS, LEFT), jnp.float32)], axis=1
                    )
                    taps = pltpu.roll(wide, CH, 1).astype(jnp.bfloat16)
                before = (cc // 2) * LEFT
                after = BAND - before - taps.shape[1]
                parts = [taps]
                if before:
                    parts = [jnp.zeros((MAPS, before), jnp.bfloat16)] + parts
                if after:
                    parts = parts + [jnp.zeros((MAPS, after), jnp.bfloat16)]
                banded[block, cc * MAPS : (cc + 1) * MAPS, place * BAND : (place + 1) * BAND] = (
                    jnp.concatenate(parts, axis=1)
                )
        return carry

    half_taps = len(EARLY) * BAND

    def product(h, block, slots, taps):
        at = slice(h * span, (h + 1) * span)
        lanes = pl.multiple_of(block * (CB * CH), CB * CH)
        patches = jnp.concatenate([x[d][at, pl.ds(lanes, BAND)] for d in slots], axis=1)
        return lax.dot_general(
            banded[block, :, taps],
            patches,
            (((1,), (1,)), ((), ())),
            preferred_element_type=jnp.float32,
        )

    def early(h):
        handed(h, (0, 4))

        def one_block(block, carry):
            partial[h, block] = product(h, block, EARLY, slice(0, half_taps))
            of_block = pl.ds(pl.multiple_of(block * (CB * MAPS), CB * MAPS), CB * MAPS)
            of_piece = slice(h * piece, (h + 1) * piece)
            wanted[h, of_block, :] = jnp.concatenate(
                [targets[p, of_block, of_piece].astype(jnp.float32) for p in range(POOL)], axis=1
            ).astype(jnp.bfloat16)
            return carry

        lax.fori_loop(0, REPS, one_block, 0)
        own_window(h, EARLY)

    def forward(h, low, high):
        def one_block(block, carry):
            total = partial[h, block] + product(h, block, LATE, slice(half_taps, 2 * half_taps))
            active = jnp.tanh(FACTOR * total)
            of_block = pl.ds(pl.multiple_of(block * (CB * MAPS), CB * MAPS), CB * MAPS)
            gap = active - wanted[h, of_block, :].astype(jnp.float32)
            signal[block] = (gap * (1.0 - active * active)).astype(jnp.bfloat16)
            return carry

        lax.fori_loop(low, high, one_block, 0)

    strip = 32

    def select(h):
        def one_strip(i, carry):
            at = pl.ds(pl.multiple_of(i * strip, strip), strip)
            parts = [signal[block, at, :] for block in range(REPS)]
            results = []
            for k in range(REPS):
                taken = None
                for block in range(REPS):
                    scale = jnp.full((strip, span), pick[k][block], jnp.float32)
                    term = scale.astype(jnp.bfloat16) * parts[block]
                    taken = term if taken is None else taken + term
                results.append(taken)
            own[h, at, :] = results[0]
            chosen[h, 0, at, :] = results[1]
            kept[h, at, :] = results[2]
            chosen[h, 1, at, :] = results[3]
            return carry

        lax.fori_loop(0, CB * MAPS // strip, one_strip, 0)
        choice(h).start()

    def choice(h):
        return pltpu.make_async_remote_copy(
            src_ref=chosen.at[h],
            dst_ref=chosen_in.at[h],
            send_sem=send_s.at[h],
            recv_sem=recv_s.at[h],
            device_id=sibling,
            device_id_type=MESH,
        )

    def pair_copy(h):
        return pltpu.make_async_remote_copy(
            src_ref=pair.at[h],
            dst_ref=pair_in.at[h],
            send_sem=send_p.at[h],
            recv_sem=recv_p.at[h],
            device_id=partner,
            device_id_type=MESH,
        )

    def make_pair(h):
        choice(h).wait_recv()

        def one_strip(i, carry):
            at = pl.ds(pl.multiple_of(i * strip, strip), strip)
            pair[h, at, :] = (
                count[0] * kept[h, at, :].astype(jnp.float32)
                + count[1] * chosen_in[h, 1, at, :].astype(jnp.float32)
            ).astype(jnp.bfloat16)
            return carry

        lax.fori_loop(0, CB * MAPS // strip, one_strip, 0)
        pair_copy(h).start()

    def combine(h):
        pair_copy(h).wait_recv()

        def one_strip(i, carry):
            at = pl.ds(pl.multiple_of(i * strip, strip), strip)
            combined[at, h * span : (h + 1) * span] = (
                count[0] * own[h, at, :].astype(jnp.float32)
                + count[1] * chosen_in[h, 0, at, :].astype(jnp.float32)
                + pair_in[h, at, :].astype(jnp.float32)
            ).astype(jnp.bfloat16)
            return carry

        lax.fori_loop(0, CB * MAPS // strip, one_strip, 0)

    def own_window(h, slots):
        def one_strip(i, carry):
            at = pl.ds(pl.multiple_of(h * span + i * strip, strip), strip)
            for d in slots:
                taken = None
                for block in range(REPS):
                    scale = jnp.full((strip, BAND), pick[0][block], jnp.float32)
                    lanes = slice(block * CB * CH, block * CB * CH + BAND)
                    term = scale.astype(jnp.bfloat16) * x[d][at, lanes]
                    taken = term if taken is None else taken + term
                window[d, at, :] = taken
            return carry

        lax.fori_loop(0, span // strip, one_strip, 0)

    def finish(h):
        last_rows(h)
        forward(h, 0, REPS // 2)
        if h:
            make_pair(h - 1)
        forward(h, REPS // 2, REPS)
        select(h)
        own_window(h, LATE)

    for h in range(PIECES):
        natives(h)
    loads[0].wait()
    lax.fori_loop(0, REPS, band_weights, 0)
    for load in loads[1:]:
        load.wait()
    below_first(0)
    below_first(1)
    straight(0)
    below_second(0)
    below_first(2)
    below_second(1)
    below_first(3)
    straight(1)
    below_second(2)
    below_second(3)
    for h in range(PIECES):
        above(h)
    early(0)
    crossed(0, 0)
    crossed(0, 1)
    straight(2)
    early(1)
    crossed(1, 0)
    crossed(0, 2)
    straight(3)
    early(2)
    crossed(1, 1)
    early(3)
    crossed(0, 3)
    finish(0)
    crossed(1, 2)
    finish(1)
    crossed(1, 3)
    finish(2)
    finish(3)
    make_pair(PIECES - 1)
    for h in range(PIECES):
        combine(h)

    def part_of(ref, d):
        return ref.at[:, :, pl.ds(d * TAPS, TAPS)]

    def block_copy(source, target, d, device, sems):
        return pltpu.make_async_remote_copy(
            src_ref=part_of(fetched_ref.at[source], d),
            dst_ref=part_of(fetched_ref.at[target], d),
            send_sem=send_w.at[sems, d],
            recv_sem=recv_w.at[sems, d],
            device_id=device,
            device_id_type=MESH,
        )

    def send_across(d):
        return block_copy(0, 2, d, partner, 0)

    def send_beside(d):
        return block_copy(0, 1, d, sibling, 1)

    def pass_beside(d):
        return block_copy(2, 3, d, sibling, 2)

    def send_part(d):
        send_across(d).start()
        send_beside(d).start()

    for d in range(FIELD):
        for at in range(0, BAND, 256):
            wide = min(256, BAND - at)
            grad[:, at : at + wide] = jnp.dot(
                combined[...],
                window[d, :, at : at + wide],
                preferred_element_type=jnp.float32,
            )
        if d:
            send_part(d - 1)
        for cc in range(CB):
            before = (cc // 2) * LEFT
            of_column = slice(cc * MAPS, (cc + 1) * MAPS)
            if cc % 2:
                wide = grad[of_column, before : before + TAPS + LEFT]
                column = pltpu.roll(wide, TAPS + LEFT - CH, 1)[:, :TAPS]
            else:
                column = grad[of_column, before : before + TAPS]
            slot_grad = FACTOR * column
            taps = slice(d * TAPS, (d + 1) * TAPS)
            accum_next = accum_out[cc, :, taps] + slot_grad * slot_grad
            master_next = master_out[cc, :, taps] - LEARNING_RATE * slot_grad / (
                jnp.sqrt(accum_next) + EPSILON
            )
            accum_out[cc, :, taps] = accum_next
            master_out[cc, :, taps] = master_next
            fetched_ref[0, cc, :, taps] = master_next.astype(jnp.bfloat16)

    send_part(FIELD - 1)
    for d in range(FIELD):
        send_across(d).wait_recv()
        pass_beside(d).start()

    for d in range(FIELD):
        send_across(d).wait_send()
        send_beside(d).wait()
        pass_beside(d).wait()
    pieces = range(PIECES)
    for h in pieces:
        choice(h).wait_send()
        pair_copy(h).wait_send()

    def all_sent(condition, sems):
        @pl.when(condition)
        def _():
            for sem in sems:
                link(OWN, OWN, 0, 0, partner, sem).wait_send()

    all_sent(has_ahead, [send_a.at[i, h] for i in (0, 1) for h in pieces])
    all_sent(has_behind, [send_b.at[1, h] for h in pieces])
    all_sent(s >= 0, [send_c.at[0, h] for h in pieces])
    all_sent(odd == 1, [send_c.at[1, h] for h in pieces])
    all_sent(s == 1, [send_b.at[0, h] for h in pieces])
    all_sent((even & has_ahead) | ((odd == 1) & has_behind), [send_d.at[0, h] for h in pieces])
    all_sent(even & has_ahead, [send_d.at[1, h] for h in pieces])
    all_sent(has_ahead, [send_e.at[h] for h in pieces])
    all_sent(has_behind & valid[3], [send_f.at[i, h] for i in (0, 1) for h in pieces])
    all_sent(valid[4], [send_g.at[h] for h in pieces])
    for slot in (0, 1, 3, 4, 5):
        all_sent(valid[slot], [send_x.at[slot, j, h] for j in (0, 1) for h in pieces])


def place_kernel(
    owner_ref, fetched, master, accum, working_out, master_out, accum_out, sem_out
):
    g = lax.axis_index("rep")
    moves = []
    for block in range(REPS):
        owner = 0
        for i in range(REPS):
            owner = jnp.where(owner_ref[i] == block, i, owner)
        k = 2 * ((owner // 2 + g // 2) % 2) + (owner + g) % 2
        for cc in range(0, CB, 2):
            moves.append(
                (fetched.at[k, pl.ds(cc, 2)], working_out.at[pl.ds(block * CB + cc, 2)])
            )
    for cc in range(CB):
        moves.append((master.at[cc], master_out.at[cc]))
        moves.append((accum.at[cc], accum_out.at[cc]))
    copies = [pltpu.make_async_copy(a, b, sem_out.at[i]) for i, (a, b) in enumerate(moves)]
    for copy in copies:
        copy.start()
    for copy in copies:
        copy.wait()


def per_device(
    working, master_slots, accum_slots, pool_images, pool_targets, batch_index, owner_map
):
    sites = lax.axis_size("site")
    batch = pool_images.shape[1]
    width = pool_images.shape[3]
    weights = working[0, 0]
    columns, maps, kdim = weights.shape
    padded = width - CB * CH + BAND
    span = POOL * (batch // PIECES)
    any_space = pl.BlockSpec(memory_space=pl.ANY)
    smem = pl.BlockSpec(memory_space=pltpu.SMEM)
    vmem = pl.BlockSpec(memory_space=pltpu.VMEM)
    dma = pltpu.SemaphoreType.DMA
    fetched, master_next, accum_next = pl.pallas_call(
        functools.partial(step_kernel, sites),
        out_shape=(
            pltpu.VMEM((REPS, CB, maps, kdim), jnp.bfloat16),
            pltpu.VMEM((CB, maps, kdim), jnp.float32),
            pltpu.VMEM((CB, maps, kdim), jnp.float32),
        ),
        in_specs=[smem, smem] + [any_space] * 5,
        out_specs=(vmem, vmem, vmem),
        scratch_shapes=[pltpu.VMEM((POOL * batch, padded), jnp.bfloat16)] * FIELD
        + [
            pltpu.VMEM((columns, maps, kdim), jnp.bfloat16),
            pltpu.VMEM((REPS, CB * maps, FIELD * BAND), jnp.bfloat16),
            pltpu.VMEM((POOL, columns * maps, batch), jnp.bfloat16),
            pltpu.VMEM((REPS, CB * maps, span), jnp.bfloat16),
            pltpu.VMEM((PIECES, 2, CB * maps, span), jnp.bfloat16),
            pltpu.VMEM((PIECES, 2, CB * maps, span), jnp.bfloat16),
            pltpu.VMEM((PIECES, CB * maps, span), jnp.bfloat16),
            pltpu.VMEM((PIECES, CB * maps, span), jnp.bfloat16),
            pltpu.VMEM((PIECES, CB * maps, span), jnp.bfloat16),
            pltpu.VMEM((PIECES, CB * maps, span), jnp.bfloat16),
            pltpu.VMEM((CB * maps, POOL * batch), jnp.bfloat16),
            pltpu.VMEM((FIELD, POOL * batch, BAND), jnp.bfloat16),
            pltpu.VMEM((PIECES, REPS, CB * maps, span), jnp.float32),
            pltpu.VMEM((PIECES, columns * maps, span), jnp.bfloat16),
            pltpu.VMEM((CB * maps, BAND), jnp.float32),
            dma((POOL + 4, PIECES)),
            dma((2, PIECES)),
            dma((2, PIECES)),
            dma((2, PIECES)),
            dma((2, PIECES)),
            dma((PIECES,)),
            dma((2, PIECES)),
            dma((PIECES,)),
            dma((FIELD, 2, PIECES)),
            dma((FIELD, 2, PIECES)),
            dma((FIELD, 2, PIECES)),
            dma((PIECES,)),
            dma((PIECES,)),
            dma((PIECES,)),
            dma((PIECES,)),
            dma((3, FIELD)),
            dma((3, FIELD)),
        ],
        compiler_params=pltpu.CompilerParams(
            collective_id=0, has_side_effects=True, vmem_limit_bytes=52 * 1024 * 1024
        ),
        name="step",
    )(
        batch_index,
        owner_map,
        pool_images[:, :, 0, :],
        pool_targets.reshape(POOL, columns * maps, batch),
        weights,
        master_slots[0, 0],
        accum_slots[0, 0],
    )
    working_next, master_next, accum_next = pl.pallas_call(
        place_kernel,
        out_shape=(
            jax.ShapeDtypeStruct((columns, maps, kdim), jnp.bfloat16),
            jax.ShapeDtypeStruct((CB, maps, kdim), jnp.float32),
            jax.ShapeDtypeStruct((CB, maps, kdim), jnp.float32),
        ),
        in_specs=[smem, vmem, vmem, vmem],
        out_specs=(any_space, any_space, any_space),
        scratch_shapes=[dma((4 * CB,))],
        compiler_params=pltpu.CompilerParams(vmem_limit_bytes=16 * 1024 * 1024),
        name="place",
    )(owner_map, fetched, master_next, accum_next)
    working_next = working_next[None]
    return (working_next, master_next[None, None], accum_next[None, None])


def solution(mesh):
    placed = (
        P("rep", "site", None, None, None),
        P("site", "rep", None, None, None),
        P("site", "rep", None, None, None),
        P(None, None, "site", None),
        P(None, "site", None, None, None),
        P(),
        P(),
    )
    return jax.shard_map(
        per_device,
        mesh=mesh,
        in_specs=placed,
        out_specs=(
            P("site", None, None, None),
            P("site", "rep", None, None, None),
            P("site", "rep", None, None, None),
        ),
        check_vma=False,
    )
```
